32 devices in a mesh: groups: 2 (over y), rows: 4 (over z), cols: 2 (over x), sub: 2 (over core).
Axes of the slice: x: 2, y: 2, z: 4, core: 2. Of those that a mesh axis runs over, the one named last changes fastest.
Arguments:
- returns: float32 [8, 64, 8192], P('groups', 'rows', ('cols', 'sub')), parts along dimension 0, may hold values from -6 to 6
- starts: int32 [8, 8192], P('groups', ('cols', 'sub')), parts along dimension 0, may hold values from 0 to 32
- start_block: float32 [8, 32, 8192], P('groups', None, ('cols', 'sub')), parts along dimension 0, may hold values from -6 to 6
Outputs:
- loadings: float32 [8, 32, 8192], P('groups', None, ('cols', 'sub')), parts along dimension 0
The draws below stay inside these ranges and needn't reach their ends.
There are 2 independent parts, one for each index of `groups`. The reference program is written for one: setup_inputs(seed, part) draws one part's arguments, and reference() takes and returns one part's arrays. A program takes and returns all parts, laid end to end along the dimension named above; each array names one. Nothing has to cross between parts.
Inputs may be any that keep to these rules, and one draw needn't show every extreme that they name: `starts`: days before an asset's start day hold returns that do not count.
All inputs are finite; a program needn't handle non-finite values.
Results may differ from the reference program's by a relative error of at most 0.0078.
Values may be sent and summed in bfloat16 or wider, within the bound.
A program may use at most 64 MiB of HBM per device.

```python
import jax
import jax.numpy as jnp
from jax import lax

ASSETS = 8192
K = 32
ITERS = 3
NWIN = 4
TIME = 64


def place_ends(array, rng, low, top_value):
    dims = array.shape
    index_at = [jax.random.randint(jax.random.fold_in(rng, axis), (), 0, dims[axis]) for axis in range(len(dims))]
    array = array.at[tuple(index_at)].set(low)
    longest = dims.index(max(dims))
    index_at[longest] = (index_at[longest] + 1) % dims[longest]
    return array.at[tuple(index_at)].set(top_value)


def block_scale(own_key, extent, cuts, least, high):
    def one(dim, parts):
        heights = jax.random.uniform(jax.random.fold_in(jax.random.fold_in(own_key, 6), dim), (parts,), jnp.float32, least / len(cuts), high / len(cuts))
        return jnp.repeat(jnp.exp(heights), extent[dim] // parts).reshape((-1,) + (1,) * (len(extent) - dim - 1))

    gain = one(*cuts[0])
    for cut in cuts[1:]:
        gain = gain * one(*cut)
    return gain


def noise(own_key, shape, width, limit, shards=(), kind=jnp.bfloat16):
    level = block_scale(own_key, shape, shards, -0.22, 0.18) if shards else 1.0
    array = jax.random.normal(own_key, shape, jnp.float32) * width * level
    return jnp.minimum(jnp.maximum(array, -limit), limit).astype(kind)


def setup_inputs(seed: int = 0, part: int = 0) -> dict:
    key_list = jax.random.split(jax.random.key(seed), 4)
    own_keys = jax.random.split(jax.random.fold_in(key_list[3], part), 4)
    returns = noise(own_keys[0], (NWIN, TIME, ASSETS), 1.0, 6.0, ((1, 4), (2, 4)), jnp.float32)
    starts = place_ends(jax.random.randint(own_keys[1], (NWIN, ASSETS), 0, TIME // 2 + 1), jax.random.fold_in(own_keys[1], 1), 0, (TIME // 2 + 1) - 1).astype(jnp.int32)
    start_block = noise(own_keys[2], (NWIN, K, ASSETS), 1.0, 6.0, ((2, 4),), jnp.float32)
    return dict(returns=returns, starts=starts, start_block=start_block)


def standardize(returns, starts):
    days = jnp.arange(TIME, dtype=jnp.int32)
    live = (days[None, :, None] >= starts[:, None, :]).astype(jnp.float32)
    counts = (TIME - starts).astype(jnp.float32)
    mean = lax.optimization_barrier(jnp.sum(live * returns, axis=1)) / counts
    centered = live * (returns - mean[:, None, :])
    squares = lax.optimization_barrier(jnp.sum(centered * centered, axis=1))
    return (centered * lax.rsqrt(squares + 1.0)[:, None, :]).astype(jnp.bfloat16)

def one_window(pair):
    scaled, factors = pair
    widened = scaled.astype(jnp.float32)
    for step in range(ITERS):
        rounded = factors.astype(jnp.bfloat16)
        proj = jnp.dot(rounded.astype(jnp.float32), scaled.T.astype(jnp.float32), preferred_element_type=jnp.float32)
        image = jnp.dot(proj, widened, precision=lax.Precision.HIGHEST)
        gram = jnp.dot(image, image.T, precision=lax.Precision.HIGHEST) / ASSETS
        lower = jnp.linalg.cholesky(gram)
        factors = jax.scipy.linalg.solve_triangular(lower, image, lower=True)
    return factors

def reference(returns, starts, start_block):
    scaled = standardize(returns, starts)
    return lax.map(one_window, (scaled, start_block))
```

```python
import functools

import jax
import jax.numpy as jnp
from jax import lax
from jax.experimental import pallas as pl
from jax.experimental.pallas import tpu as pltpu
from jax.sharding import PartitionSpec as P

ITERS = 3
HIGHEST = lax.Precision.HIGHEST
MESH = pl.DeviceIdType.MESH
NT = (((1,), (1,)), ((), ()))
SUBLANES = 8
LANES = 128
LIMIT = 6.0
TOP = 32767.0
COARSE = 32000.0


def eliminate(gram, right):
    size = gram.shape[0]
    height = min(SUBLANES, size)
    blocks = size // height
    gs = [gram[b * height:(b + 1) * height] for b in range(blocks)]
    rs = [right[b * height:(b + 1) * height] for b in range(blocks)]
    row_id = lax.broadcasted_iota(jnp.int32, (height, 1), 0)
    diag = [jnp.ones((height, right.shape[1]), jnp.float32) for _ in range(blocks)]
    wide = max(size, right.shape[1])
    for b in range(blocks):
        panel = {
            (c, i): jnp.broadcast_to(gs[c][:, b * height + i:b * height + i + 1], (height, wide))
            for c in range(b, blocks) for i in range(height)
        }
        for i in range(height):
            grow = gs[b][i:i + 1]
            rrow = rs[b][i:i + 1]
            pivot = panel[b, i][i:i + 1]
            diag[b] = jnp.where(row_id == i, pivot[:, :right.shape[1]], diag[b])
            inverse = 1.0 / pivot
            ahead = {n: panel[b, n][i:i + 1] for n in range(i + 1, height)}
            for c in range(b, blocks):
                factor = panel[c, i] * inverse
                if c == b:
                    factor = jnp.where(row_id > i, factor, 0.0)
                for n in range(i + 1, height):
                    panel[c, n] = panel[c, n] - factor * ahead[n]
                gs[c] = gs[c] - factor[:, :size] * grow
                rs[c] = rs[c] - factor[:, :right.shape[1]] * rrow
    return jnp.concatenate([r * lax.rsqrt(d) for r, d in zip(rs, diag)], axis=0)


def kernel(rows, cols, subs, assets,
           returns_ref, starts_ref, start_ref, out_ref,
           held, begins, firsts, codes, lhs, sbuf, mine, quad, mloc, mall,
           ls, bs, cs, cr, qs, qr, ms, mr):
    r = lax.axis_index("rows")
    mates = cols * subs
    m = lax.axis_index("cols") * subs + lax.axis_index("sub")
    windows, days, width = returns_ref.shape
    k = start_ref.shape[1]
    total = days * rows
    groups = width // LANES
    half = (k + total) // 2
    ends = ((0, 1), (rows - 1, rows - 2))

    def row_peer(d):
        return lax.rem(r + d, rows)

    def mate(d):
        return lax.rem(m + d, mates)

    def row_id(q):
        return {"rows": q}

    def mate_id(q):
        return {"cols": q // subs, "sub": lax.rem(q, subs)}

    def lanes(g):
        return slice(g * LANES, (g + 1) * LANES)

    load_begins = [pltpu.make_async_copy(starts_ref.at[pl.ds(w, 1)], begins.at[w], bs.at[w]) for w in range(windows)]
    for c in load_begins:
        c.start()
    loads = [pltpu.make_async_copy(returns_ref.at[w], held.at[w], ls.at[w]) for w in range(windows)]
    for c in loads:
        c.start()
    load_firsts = pltpu.make_async_copy(start_ref.at[r], firsts, bs.at[windows])
    load_firsts.start()

    barrier = pltpu.get_barrier_semaphore()
    for d in range(1, rows):
        pl.semaphore_signal(barrier, inc=1, device_id=row_id(row_peer(d)), device_id_type=MESH)
    for d in range(1, mates):
        pl.semaphore_signal(barrier, inc=1, device_id=mate_id(mate(d)), device_id_type=MESH)

    row = lax.broadcasted_iota(jnp.int32, (groups, LANES), 0)
    own_day = r * days + lax.broadcasted_iota(jnp.int32, (days, LANES), 0)
    for w in range(windows):
        load_begins[w].wait()
        loads[w].wait()
        centers = jnp.zeros((groups, LANES), jnp.float32)
        scales = jnp.zeros((groups, LANES), jnp.float32)
        for g in range(groups):
            x = held[w, :, lanes(g)]
            x = jnp.where(own_day >= begins[w, :, lanes(g)], x, x[days - 1:days])
            top = jnp.max(x, axis=0, keepdims=True)
            low = jnp.min(x, axis=0, keepdims=True)
            center = jnp.round((top + low) * (0.5 * TOP / LIMIT))
            middle = center * (LIMIT / TOP)
            reach = jnp.maximum(top - middle, middle - low)
            scale = jnp.floor(reach * (COARSE / LIMIT)) + 1.0
            inverse = (TOP * COARSE / LIMIT) / scale
            codes[r, w, g] = jnp.round((x - middle) * inverse).astype(jnp.int32).astype(jnp.int16)
            centers = jnp.where(row == g, center, centers)
            scales = jnp.where(row == g, scale, scales)
        codes[r, w, groups] = centers.astype(jnp.int32).astype(jnp.int16)
        codes[r, w, groups + 1] = scales.astype(jnp.int32).astype(jnp.int16)

    def unit(s, w, q):
        return pltpu.make_async_remote_copy(
            src_ref=codes.at[s, w], dst_ref=codes.at[s, w], send_sem=cs.at[s, w, q],
            recv_sem=cr.at[s, w], device_id=row_id(q), device_id_type=MESH)

    def sides(t, act):
        for sign in (1, -1):
            q = r + sign * t

            @pl.when(jnp.logical_and(q >= 0, q < rows))
            def _():
                act(q)

    def own_units(act):
        for t in range(rows - 1, 0, -1):
            sides(t, lambda q: act(r, q, q))

        def rest(q, t):
            far = jnp.where(q > r, rows - 1, 0)

            @pl.when(jnp.logical_or(t == 1, jnp.logical_and(q > 0, q < rows - 1)))
            def _():
                for d in range(windows):
                    w = lax.rem(far + 1 + d, windows)

                    @pl.when(w != q)
                    def _():
                        act(r, w, q)

        for t in range(rows - 1, 0, -1):
            sides(t, lambda q: rest(q, t))

    def relayed(e, own):
        near = 1 if e == 0 else rows - 2
        pairs = [(s, w) for w in range(windows) if w != e
                 for s in range(rows) if s not in (e, near)]
        return [p for p in pairs if (p[1] == near) == own]

    def forward(part, parts):
        for e, near in ends:
            @pl.when(r == near)
            def _():
                pairs = relayed(e, False)
                for s, w in pairs[part * len(pairs) // parts:(part + 1) * len(pairs) // parts]:
                    unit(s, w, e).wait_recv()
                    unit(s, w, e).start()

    def relays(s, w):
        flags = [jnp.logical_and(r == near, jnp.logical_and(s != e, w != e)) for e, near in ends]
        return functools.reduce(jnp.logical_or, flags)

    pl.semaphore_wait(barrier, rows - 1 + mates - 1)
    own_units(lambda s, w, q: unit(s, w, q).start())

    load_firsts.wait()
    lhs[:k] = firsts[...].astype(jnp.bfloat16)

    day = lax.broadcasted_iota(jnp.int32, (total, LANES), 0)

    def standardize(w, store):
        middles, steps = [], []
        for s in range(rows):
            middles.append(codes[s, w, groups].astype(jnp.float32) * (LIMIT / TOP))
            steps.append(codes[s, w, groups + 1].astype(jnp.float32) * (LIMIT / TOP / COARSE))
        for g in range(groups):
            x = jnp.concatenate([
                codes[s, w, g].astype(jnp.float32) * steps[s][g:g + 1] + middles[s][g:g + 1]
                for s in range(rows)], axis=0)
            begin = begins[w, :, lanes(g)]
            live = day >= begin
            counts = (total - begin).astype(jnp.float32)
            mean = jnp.sum(jnp.where(live, x, 0.0), axis=0, keepdims=True) / counts
            centered = jnp.where(live, x - mean, 0.0)
            squares = jnp.sum(centered * centered, axis=0, keepdims=True)
            store(g, (centered * lax.rsqrt(squares + 1.0)).astype(jnp.bfloat16))

    for d in range(1, rows):
        unit(row_peer(d), r, r).wait_recv()
    for e, near in ends:
        @pl.when(r == near)
        def _():
            for s, w in relayed(e, True):
                unit(s, w, e).start()

    def keep_own(g, value):
        lhs[k:, lanes(g)] = value

    standardize(r, keep_own)
    sums = lax.dot_general(lhs[...], lhs[k:], NT, preferred_element_type=jnp.float32)
    summed = jnp.concatenate([sums[:half], sums[half:]], axis=1)
    mine[...] = summed
    sends = []
    for d in range(1, mates):
        q = mate(d)
        c = pltpu.make_async_remote_copy(
            src_ref=mine, dst_ref=quad.at[m], send_sem=qs.at[d], recv_sem=qr.at[m],
            device_id=mate_id(q), device_id_type=MESH)
        c.start()
        sends.append(c)
    quad[m] = summed
    forward(0, 2)
    for d in range(1, mates):
        q = mate(d)
        pltpu.make_async_remote_copy(
            src_ref=mine, dst_ref=quad.at[q], send_sem=qs.at[d], recv_sem=qr.at[q],
            device_id=mate_id(q), device_id_type=MESH).wait_recv()
    both = quad[0]
    for q in range(1, mates):
        both = both + quad[q]
    both = jnp.concatenate([both[:, :total], both[:, total:]], axis=0)
    proj, corr = both[:k], both[k:]
    for step in range(ITERS):
        image = jnp.dot(proj, corr, precision=HIGHEST, preferred_element_type=jnp.float32)
        gram = lax.dot_general(image, proj, NT, precision=HIGHEST,
                               preferred_element_type=jnp.float32) / assets
        proj = eliminate(gram, image if step < ITERS - 1 else proj)
        if step == 0:
            forward(1, 2)
    mloc[...] = proj
    mall[r] = proj

    def deliver(q, slot):
        return pltpu.make_async_remote_copy(
            src_ref=mloc, dst_ref=mall.at[slot], send_sem=ms.at[q], recv_sem=mr.at[slot],
            device_id=row_id(q), device_id_type=MESH)

    for t in range(rows - 1, 0, -1):
        sides(t, lambda q: deliver(q, r).start())

    def finish(w, scaled):
        value = mall[w]
        high = value.astype(jnp.bfloat16)
        low = (value - high.astype(jnp.float32)).astype(jnp.bfloat16)
        wide = jnp.dot(jnp.concatenate([high, low], axis=0), scaled,
                       preferred_element_type=jnp.float32)
        out_ref[w] = wide[:k] + wide[k:]

    finish(r, lhs[k:])
    for d in range(1, rows):
        w = row_peer(d)
        for b in range(1, rows):
            s = row_peer(b)

            @pl.when(jnp.logical_not(relays(s, w)))
            def _():
                unit(s, w, r).wait_recv()

        def keep(g, value):
            sbuf[w, :, lanes(g)] = value

        standardize(w, keep)
    for d in range(1, rows):
        w = row_peer(d)
        deliver(w, w).wait_recv()
        finish(w, sbuf[w])
    for c in sends:
        c.wait_send()
    own_units(lambda s, w, q: unit(s, w, q).wait_send())
    for e, near in ends:
        @pl.when(r == near)
        def _():
            for s, w in relayed(e, True) + relayed(e, False):
                unit(s, w, e).wait_send()
    for t in range(rows - 1, 0, -1):
        sides(t, lambda q: deliver(q, r).wait_send())


def fused(returns, starts, start_block, rows, cols, subs):
    windows, days, width = returns.shape
    k = start_block.shape[1]
    total = days * rows
    mates = cols * subs
    half = (k + total) // 2
    groups = width // LANES
    f32, bf16 = jnp.float32, jnp.bfloat16
    dma = pltpu.SemaphoreType.DMA
    return pl.pallas_call(
        functools.partial(kernel, rows, cols, subs, width * mates),
        out_shape=pltpu.VMEM(start_block.shape, f32),
        in_specs=[pl.BlockSpec(memory_space=pl.ANY)] * 3,
        out_specs=pl.BlockSpec(memory_space=pltpu.VMEM),
        scratch_shapes=[
            pltpu.VMEM(returns.shape, f32),
            pltpu.VMEM((windows, 1, width), jnp.int32),
            pltpu.VMEM((k, width), f32),
            pltpu.VMEM((rows, windows, groups + 2, days, LANES), jnp.int16),
            pltpu.VMEM((k + total, width), bf16),
            pltpu.VMEM((windows, total, width), bf16),
            pltpu.VMEM((half, 2 * total), f32),
            pltpu.VMEM((mates, half, 2 * total), f32),
            pltpu.VMEM((k, total), f32),
            pltpu.VMEM((windows, k, total), f32),
            dma((windows,)), dma((windows + 1,)),
            dma((rows, windows, rows)), dma((rows, windows)),
            dma((mates,)), dma((mates,)),
            dma((rows,)), dma((rows,)),
        ],
        compiler_params=pltpu.CompilerParams(collective_id=0, has_side_effects=True),
    )(returns, starts, start_block)


def gram_of(image):
    return jnp.einsum("wkj,wlj->wkl", image, image, precision=HIGHEST)


def project(factors, scaled):
    rounded = factors.astype(jnp.bfloat16)
    return jnp.einsum("wka,wta->wkt", rounded, scaled, preferred_element_type=jnp.float32)


def expand(proj, widened):
    return jnp.einsum("wkt,wta->wka", proj, widened, precision=HIGHEST)


def orthonormal(image, gram, assets):
    lower = jnp.linalg.cholesky(gram / assets)
    return jax.scipy.linalg.solve_triangular(lower, image, lower=True)


def stepwise(returns, starts, start_block, rows, mates):
    windows, days, width = returns.shape
    row_pos = lax.axis_index("rows")
    total_days = days * rows
    day_index = row_pos * days + jnp.arange(days, dtype=jnp.int32)
    live = (day_index[None, :, None] >= starts[:, None, :]).astype(jnp.float32)
    counts = (total_days - starts).astype(jnp.float32)
    masked = live * returns
    sums = lax.psum(jnp.sum(masked, axis=1), "rows")
    mean = sums / counts
    centered = live * (returns - mean[:, None, :])
    squares = lax.psum(jnp.sum(centered * centered, axis=1), "rows")
    scaled = (centered * lax.rsqrt(squares + 1.0)[:, None, :]).astype(jnp.bfloat16)
    widened = scaled.astype(jnp.float32)
    factors = start_block
    for step in range(ITERS):
        proj = lax.psum(project(factors, scaled), ("cols", "sub"))
        image = lax.psum(expand(proj, widened), "rows")
        gram = lax.psum(gram_of(image), ("cols", "sub"))
        factors = orthonormal(image, gram, width * mates)
    return factors


def on_device(rows, cols, subs, returns, starts, start_block):
    windows, days, width = returns.shape
    k = start_block.shape[1]
    fits = (windows == rows and width == LANES * days and days % 16 == 0 and k % 16 == 0
            and days * rows <= 64 and (days * rows + k) % 16 == 0 and rows > 3 and cols * subs > 1)
    if fits:
        return fused(returns, starts, start_block, rows, cols, subs)
    return stepwise(returns, starts, start_block, rows, cols * subs)


def solution(mesh):
    placed = (
        P("groups", "rows", ("cols", "sub")),
        P("groups", ("cols", "sub")),
        P("groups", None, ("cols", "sub")),
    )
    sizes = (mesh.shape["rows"], mesh.shape["cols"], mesh.shape["sub"])
    return jax.shard_map(
        functools.partial(on_device, *sizes),
        mesh=mesh,
        in_specs=placed,
        out_specs=P("groups", None, ("cols", "sub")),
        check_vma=False,
    )
```

```python
import functools

import jax
import jax.numpy as jnp
from jax import lax
from jax.experimental import pallas as pl
from jax.experimental.pallas import tpu as pltpu
from jax.sharding import PartitionSpec as P

ITERS = 3
HIGHEST = lax.Precision.HIGHEST
MESH = pl.DeviceIdType.MESH
NT = (((1,), (1,)), ((), ()))
SUBLANES = 8
LANES = 128
LIMIT = 6.0
TOP = 32767.0
TINY = 1e-30
EARLY = 3


def eliminate(gram, right):
    size = gram.shape[0]
    height = min(SUBLANES, size)
    blocks = size // height
    gs = [gram[b * height:(b + 1) * height] for b in range(blocks)]
    rs = [right[b * height:(b + 1) * height] for b in range(blocks)]
    row_id = lax.broadcasted_iota(jnp.int32, (height, 1), 0)
    diag = [jnp.ones((height, right.shape[1]), jnp.float32) for _ in range(blocks)]
    wide = max(size, right.shape[1])
    for b in range(blocks):
        panel = {
            (c, i): jnp.broadcast_to(gs[c][:, b * height + i:b * height + i + 1], (height, wide))
            for c in range(b, blocks) for i in range(height)
        }
        for i in range(height):
            grow = gs[b][i:i + 1]
            rrow = rs[b][i:i + 1]
            pivot = panel[b, i][i:i + 1]
            diag[b] = jnp.where(row_id == i, pivot[:, :right.shape[1]], diag[b])
            inverse = 1.0 / pivot
            ahead = {n: panel[b, n][i:i + 1] for n in range(i + 1, height)}
            for c in range(b, blocks):
                factor = panel[c, i] * inverse
                if c == b:
                    factor = jnp.where(row_id > i, factor, 0.0)
                for n in range(i + 1, height):
                    panel[c, n] = panel[c, n] - factor * ahead[n]
                gs[c] = gs[c] - factor[:, :size] * grow
                rs[c] = rs[c] - factor[:, :right.shape[1]] * rrow
    return jnp.concatenate([r * lax.rsqrt(d) for r, d in zip(rs, diag)], axis=0)


def kernel(rows, cols, subs, assets,
           returns_ref, starts_ref, start_ref, out_ref,
           held, begins, firsts, codes, lhs, sbuf, mine, quad, mloc, mall, gains,
           ls, bs, cs, cr, qs, qr, ms, mr, gs, gr, clear):
    r = lax.axis_index("rows")
    mates = cols * subs
    m = lax.axis_index("cols") * subs + lax.axis_index("sub")
    windows, days, width = returns_ref.shape
    k = start_ref.shape[1]
    total = days * rows
    groups = width // LANES
    half = (k + total) // 2
    ends = ((0, 1), (rows - 1, rows - 2))

    def row_peer(d):
        return lax.rem(r + d, rows)

    def mate(d):
        return lax.rem(m + d, mates)

    def row_id(q):
        return {"rows": q}

    def mate_id(q):
        return {"cols": q // subs, "sub": lax.rem(q, subs)}

    def lanes(g):
        return slice(g * LANES, (g + 1) * LANES)

    order = [row_peer(d) for d in sorted(range(rows), key=lambda d: -min(d, rows - d))]
    load_begins = [pltpu.make_async_copy(starts_ref.at[pl.ds(w, 1)], begins.at[w], bs.at[w]) for w in range(windows)]
    for c in load_begins:
        c.start()
    loads = [pltpu.make_async_copy(returns_ref.at[w], held.at[w], ls.at[w]) for w in order]
    for c in loads:
        c.start()
    load_firsts = pltpu.make_async_copy(start_ref.at[r], firsts, bs.at[windows])
    load_firsts.start()

    barrier = pltpu.get_barrier_semaphore()
    for d in range(1, rows):
        pl.semaphore_signal(barrier, inc=1, device_id=row_id(row_peer(d)), device_id_type=MESH)
    for d in range(1, mates):
        pl.semaphore_signal(barrier, inc=1, device_id=mate_id(mate(d)), device_id_type=MESH)

    def unit(s, w, q):
        return pltpu.make_async_remote_copy(
            src_ref=codes.at[s, w], dst_ref=codes.at[s, w], send_sem=cs.at[s, w, q],
            recv_sem=cr.at[s, w], device_id=row_id(q), device_id_type=MESH)

    def gain(s, q):
        return pltpu.make_async_remote_copy(
            src_ref=gains.at[s], dst_ref=gains.at[s], send_sem=gs.at[q],
            recv_sem=gr.at[s], device_id=row_id(q), device_id_type=MESH)

    row = lax.broadcasted_iota(jnp.int32, (groups, LANES), 0)
    own_day = r * days + lax.broadcasted_iota(jnp.int32, (days, LANES), 0)

    def encode(w):
        def load(g):
            x = held[w, :, lanes(g)]
            return jnp.where(own_day >= begins[w, :, lanes(g)], x, x[days - 1:days])

        centers = jnp.zeros((groups, LANES), jnp.float32)
        reach = jnp.full((1, LANES), TINY, jnp.float32)
        middles = []
        for g in range(groups):
            x = load(g)
            top = jnp.max(x, axis=0, keepdims=True)
            low = jnp.min(x, axis=0, keepdims=True)
            center = jnp.round((top + low) * (0.5 * TOP / LIMIT))
            middle = center * (LIMIT / TOP)
            reach = jnp.maximum(reach, jnp.maximum(top - middle, middle - low))
            centers = jnp.where(row == g, center, centers)
            middles.append(middle)
        codes[r, w, groups] = centers.astype(jnp.int32).astype(jnp.int16)
        gains[r, w] = reach * (1.0 / TOP)
        inverse = TOP / reach
        for g in range(groups):
            codes[r, w, g] = jnp.round((load(g) - middles[g]) * inverse).astype(jnp.int32).astype(jnp.int16)

    def sides(t, act):
        for sign in (1, -1):
            q = r + sign * t

            @pl.when(jnp.logical_and(q >= 0, q < rows))
            def _():
                act(q)

    def other_units(act, stages):
        def rest(q, t, right):
            end = jnp.logical_or(q == 0, q == rows - 1)
            for d in range(windows):
                w = d if right else windows - 1 - d
                inner = (1 if d == 0 else 2 if d < windows - 1 else 3) in stages
                outer = t == 1 and (0 if d < EARLY else 1) in stages
                if not inner and not outer:
                    continue
                take = q != w
                if not outer:
                    take = jnp.logical_and(take, jnp.logical_not(end))
                if not inner:
                    take = jnp.logical_and(take, end)

                @pl.when(take)
                def _():
                    act(r, w, q)

        for t in range(rows - 1, 0, -1):
            for sign in (1, -1):
                q = r + sign * t

                @pl.when(jnp.logical_and(q >= 0, q < rows))
                def _():
                    rest(q, t, sign > 0)

    def relayed(e, own):
        near = 1 if e == 0 else rows - 2
        turn = range(windows) if e else range(windows - 1, -1, -1)
        pairs = [(s, w) for w in turn if w != e for s in range(rows) if s not in (e, near)]
        return [p for p in pairs if (p[1] == near) == own]

    def forward(part, parts):
        for e, near in ends:
            @pl.when(r == near)
            def _():
                pairs = relayed(e, False)
                for s, w in pairs[part * len(pairs) // parts:(part + 1) * len(pairs) // parts]:
                    unit(s, w, e).wait_recv()
                    unit(s, w, e).start()

    def relays(s, w):
        flags = [jnp.logical_and(r == near, jnp.logical_and(s != e, w != e)) for e, near in ends]
        return functools.reduce(jnp.logical_or, flags)

    for c in load_begins:
        c.wait()
    for i, w in enumerate(order):
        loads[i].wait()
        encode(w)
        if i == 1:
            pl.semaphore_wait(barrier, rows - 1 + mates - 1)
        if i > 0:
            unit(r, order[i - 1], order[i - 1]).start()
    for d in range(1, rows):
        gain(r, row_peer(d)).start()
    other_units(lambda s, w, q: unit(s, w, q).start(), (0,))

    load_firsts.wait()
    lhs[:k] = firsts[...].astype(jnp.bfloat16)
    for w in order[:-1]:
        unit(r, w, w).wait_send()
    for d in range(1, subs):
        pl.semaphore_signal(clear, inc=1, device_id={"sub": lax.rem(lax.axis_index("sub") + d, subs)},
                            device_id_type=MESH)
    pl.semaphore_wait(clear, subs - 1)
    other_units(lambda s, w, q: unit(s, w, q).start(), (1,))

    day = lax.broadcasted_iota(jnp.int32, (total, LANES), 0)

    def standardize(w, store):
        middles = [codes[s, w, groups].astype(jnp.float32) * (LIMIT / TOP) for s in range(rows)]
        steps = [gains[s, w] for s in range(rows)]
        for g in range(groups):
            x = jnp.concatenate([
                codes[s, w, g].astype(jnp.float32) * steps[s] + middles[s][g:g + 1]
                for s in range(rows)], axis=0)
            begin = begins[w, :, lanes(g)]
            live = day >= begin
            counts = (total - begin).astype(jnp.float32)
            mean = jnp.sum(jnp.where(live, x, 0.0), axis=0, keepdims=True) / counts
            centered = jnp.where(live, x - mean, 0.0)
            squares = jnp.sum(centered * centered, axis=0, keepdims=True)
            store(g, (centered * lax.rsqrt(squares + 1.0)).astype(jnp.bfloat16))

    for d in range(1, rows):
        gain(row_peer(d), r).wait_recv()
        unit(row_peer(d), r, r).wait_recv()
    for e, near in ends:
        @pl.when(r == near)
        def _():
            for s, w in relayed(e, True):
                unit(s, w, e).start()

    def keep_own(g, value):
        lhs[k:, lanes(g)] = value

    standardize(r, keep_own)
    sums = lax.dot_general(lhs[...], lhs[k:], NT, preferred_element_type=jnp.float32)
    summed = jnp.concatenate([sums[:half], sums[half:]], axis=1)
    mine[...] = summed
    sends = []
    for d in range(1, mates):
        q = mate(d)
        c = pltpu.make_async_remote_copy(
            src_ref=mine, dst_ref=quad.at[m], send_sem=qs.at[d], recv_sem=qr.at[m],
            device_id=mate_id(q), device_id_type=MESH)
        c.start()
        sends.append(c)
    quad[m] = summed
    other_units(lambda s, w, q: unit(s, w, q).start(), (2,))
    for d in range(1, mates):
        q = mate(d)
        pltpu.make_async_remote_copy(
            src_ref=mine, dst_ref=quad.at[q], send_sem=qs.at[d], recv_sem=qr.at[q],
            device_id=mate_id(q), device_id_type=MESH).wait_recv()
    other_units(lambda s, w, q: unit(s, w, q).start(), (3,))
    forward(0, 2)
    both = quad[0]
    for q in range(1, mates):
        both = both + quad[q]
    both = jnp.concatenate([both[:, :total], both[:, total:]], axis=0)
    proj, corr = both[:k], both[k:]
    for step in range(ITERS):
        image = jnp.dot(proj, corr, precision=HIGHEST, preferred_element_type=jnp.float32)
        gram = lax.dot_general(image, proj, NT, precision=HIGHEST,
                               preferred_element_type=jnp.float32) / assets
        proj = eliminate(gram, image if step < ITERS - 1 else proj)
        if step == 1:
            forward(1, 2)
    mloc[...] = proj
    mall[r] = proj

    def deliver(q, slot):
        return pltpu.make_async_remote_copy(
            src_ref=mloc, dst_ref=mall.at[slot], send_sem=ms.at[q], recv_sem=mr.at[slot],
            device_id=row_id(q), device_id_type=MESH)

    for t in range(rows - 1, 0, -1):
        sides(t, lambda q: deliver(q, r).start())

    def finish(w, scaled):
        value = mall[w]
        high = value.astype(jnp.bfloat16)
        low = (value - high.astype(jnp.float32)).astype(jnp.bfloat16)
        wide = jnp.dot(jnp.concatenate([high, low], axis=0), scaled,
                       preferred_element_type=jnp.float32)
        out_ref[w] = wide[:k] + wide[k:]

    finish(r, lhs[k:])
    for d in range(1, rows):
        w = row_peer(d)
        for b in range(1, rows):
            s = row_peer(b)

            @pl.when(jnp.logical_not(relays(s, w)))
            def _():
                unit(s, w, r).wait_recv()

        def keep(g, value):
            sbuf[w, :, lanes(g)] = value

        standardize(w, keep)
    for d in range(1, rows):
        w = row_peer(d)
        deliver(w, w).wait_recv()
        finish(w, sbuf[w])
    for c in sends:
        c.wait_send()
    for d in range(1, rows):
        gain(r, row_peer(d)).wait_send()
    other_units(lambda s, w, q: unit(s, w, q).wait_send(), (0, 1, 2, 3))
    for e, near in ends:
        @pl.when(r == near)
        def _():
            for s, w in relayed(e, True) + relayed(e, False):
                unit(s, w, e).wait_send()
    for t in range(rows - 1, 0, -1):
        sides(t, lambda q: deliver(q, r).wait_send())


def fused(returns, starts, start_block, rows, cols, subs):
    windows, days, width = returns.shape
    k = start_block.shape[1]
    total = days * rows
    mates = cols * subs
    half = (k + total) // 2
    groups = width // LANES
    f32, bf16 = jnp.float32, jnp.bfloat16
    dma = pltpu.SemaphoreType.DMA
    return pl.pallas_call(
        functools.partial(kernel, rows, cols, subs, width * mates),
        out_shape=pltpu.VMEM(start_block.shape, f32),
        in_specs=[pl.BlockSpec(memory_space=pl.ANY)] * 3,
        out_specs=pl.BlockSpec(memory_space=pltpu.VMEM),
        scratch_shapes=[
            pltpu.VMEM(returns.shape, f32),
            pltpu.VMEM((windows, 1, width), jnp.int32),
            pltpu.VMEM((k, width), f32),
            pltpu.VMEM((rows, windows, groups + 1, days, LANES), jnp.int16),
            pltpu.VMEM((k + total, width), bf16),
            pltpu.VMEM((windows, total, width), bf16),
            pltpu.VMEM((half, 2 * total), f32),
            pltpu.VMEM((mates, half, 2 * total), f32),
            pltpu.VMEM((k, total), f32),
            pltpu.VMEM((windows, k, total), f32),
            pltpu.VMEM((rows, windows, 1, LANES), f32),
            dma((windows,)), dma((windows + 1,)),
            dma((rows, windows, rows)), dma((rows, windows)),
            dma((mates,)), dma((mates,)),
            dma((rows,)), dma((rows,)), dma((rows,)), dma((rows,)), pltpu.SemaphoreType.REGULAR,
        ],
        compiler_params=pltpu.CompilerParams(collective_id=0, has_side_effects=True),
    )(returns, starts, start_block)


def gram_of(image):
    return jnp.einsum("wkj,wlj->wkl", image, image, precision=HIGHEST)


def project(factors, scaled):
    rounded = factors.astype(jnp.bfloat16)
    return jnp.einsum("wka,wta->wkt", rounded, scaled, preferred_element_type=jnp.float32)


def expand(proj, widened):
    return jnp.einsum("wkt,wta->wka", proj, widened, precision=HIGHEST)


def orthonormal(image, gram, assets):
    lower = jnp.linalg.cholesky(gram / assets)
    return jax.scipy.linalg.solve_triangular(lower, image, lower=True)


def stepwise(returns, starts, start_block, rows, mates):
    windows, days, width = returns.shape
    row_pos = lax.axis_index("rows")
    total_days = days * rows
    day_index = row_pos * days + jnp.arange(days, dtype=jnp.int32)
    live = (day_index[None, :, None] >= starts[:, None, :]).astype(jnp.float32)
    counts = (total_days - starts).astype(jnp.float32)
    masked = live * returns
    sums = lax.psum(jnp.sum(masked, axis=1), "rows")
    mean = sums / counts
    centered = live * (returns - mean[:, None, :])
    squares = lax.psum(jnp.sum(centered * centered, axis=1), "rows")
    scaled = (centered * lax.rsqrt(squares + 1.0)[:, None, :]).astype(jnp.bfloat16)
    widened = scaled.astype(jnp.float32)
    factors = start_block
    for step in range(ITERS):
        proj = lax.psum(project(factors, scaled), ("cols", "sub"))
        image = lax.psum(expand(proj, widened), "rows")
        gram = lax.psum(gram_of(image), ("cols", "sub"))
        factors = orthonormal(image, gram, width * mates)
    return factors


def on_device(rows, cols, subs, returns, starts, start_block):
    windows, days, width = returns.shape
    k = start_block.shape[1]
    fits = (windows == rows and width == LANES * days and days % 16 == 0 and k % 16 == 0
            and days * rows <= 64 and (days * rows + k) % 16 == 0 and rows > 3 and cols * subs > 1)
    if fits:
        return fused(returns, starts, start_block, rows, cols, subs)
    return stepwise(returns, starts, start_block, rows, cols * subs)


def solution(mesh):
    placed = (
        P("groups", "rows", ("cols", "sub")),
        P("groups", ("cols", "sub")),
        P("groups", None, ("cols", "sub")),
    )
    sizes = (mesh.shape["rows"], mesh.shape["cols"], mesh.shape["sub"])
    return jax.shard_map(
        functools.partial(on_device, *sizes),
        mesh=mesh,
        in_specs=placed,
        out_specs=P("groups", None, ("cols", "sub")),
        check_vma=False,
    )
```

```python
import functools

import jax
import jax.numpy as jnp
from jax import lax
from jax.experimental import pallas as pl
from jax.experimental.pallas import tpu as pltpu
from jax.sharding import PartitionSpec as P

ITERS = 3
HIGHEST = lax.Precision.HIGHEST
MESH = pl.DeviceIdType.MESH
NT = (((1,), (1,)), ((), ()))
SUBLANES = 8
LANES = 128
LIMIT = 6.0
TOP = 32767.0
TINY = 1e-30


def eliminate(gram, rights):
    size, wide = gram.shape[0], rights[0].shape[1]
    tiles = size // SUBLANES
    sums = [[x[c * SUBLANES:(c + 1) * SUBLANES] for c in range(tiles)] for x in rights]
    row_id = lax.broadcasted_iota(jnp.int32, (SUBLANES, 1), 0)
    diag = [jnp.ones((SUBLANES, wide), jnp.float32) for _ in range(tiles)]
    panel = {
        (c, i): jnp.broadcast_to(gram[c * SUBLANES:(c + 1) * SUBLANES, i:i + 1], (SUBLANES, wide))
        for i in range(size) for c in range(i // SUBLANES, tiles)
    }
    for i in range(size):
        own, sub = i // SUBLANES, i % SUBLANES
        pivot = panel[own, i][sub:sub + 1]
        inverse = 1.0 / pivot
        diag[own] = jnp.where(row_id == sub, pivot, diag[own])
        ahead = {n: panel[n // SUBLANES, i][n % SUBLANES:n % SUBLANES + 1] for n in range(i + 1, size)}
        rows = [x[own][sub:sub + 1] for x in sums]
        for c in range(own, tiles):
            factor = panel[c, i] * inverse
            if c == own:
                factor = jnp.where(row_id > sub, factor, 0.0)
            for n in range(i + 1, size):
                if c >= n // SUBLANES:
                    panel[c, n] = panel[c, n] - factor * ahead[n]
            for x, row in zip(sums, rows):
                x[c] = x[c] - factor * row
    roots = [lax.rsqrt(d) for d in diag]
    return [jnp.concatenate([v * d for v, d in zip(x, roots)], axis=0) for x in sums]


def exact(left, right):
    return jnp.dot(left, right, precision=HIGHEST, preferred_element_type=jnp.float32)


def background(rows, windows, x):
    plan = []
    for q in range(rows):
        end = q in (0, rows - 1)
        if q == x or (end and abs(q - x) > 1):
            continue
        for d in range(windows):
            w = d if q > x else windows - 1 - d
            if w != q:
                plan.append((x, w, q, 0 if end else 1 if d == 0 else 3 if d == windows - 1 else 2))
    for e, near in ((0, 1), (rows - 1, rows - 2)):
        if x == near:
            far = [s for s in range(rows) if s not in (e, near)]
            plan += [(s, near, e, 4) for s in far]
            turn = [w for w in (range(windows) if e else range(windows - 1, -1, -1)) if w not in (e, near)]
            plan += [(s, w, e, 5 + i * 2 // len(turn)) for i, w in enumerate(turn) for s in far]
    return plan


def block(count, rows, windows):
    sides = [(a, count // a) for a in range(1, rows + 1) if count % a == 0 and count // a <= windows]
    return sides[0] if sides else None


def kernel(rows, cols, subs, assets,
           returns_ref, starts_ref, start_ref, out_ref,
           held, begins, firsts, codes, lhs, sbuf, mine, quad, mix, gains,
           ls, bs, cs, cr, qs, qr, ms, mr, gs, gr, rest, clear):
    r = lax.axis_index("rows")
    mates = cols * subs
    m = lax.axis_index("cols") * subs + lax.axis_index("sub")
    windows, days, width = returns_ref.shape
    k = start_ref.shape[1]
    total = days * rows
    groups = width // LANES
    half = (k + total) // 2
    ends = ((0, 1), (rows - 1, rows - 2))

    def row_peer(d):
        return lax.rem(r + d, rows)

    def mate(d):
        return lax.rem(m + d, mates)

    def row_id(q):
        return {"rows": q}

    def mate_id(q):
        return {"cols": q // subs, "sub": lax.rem(q, subs)}

    def lanes(g):
        return slice(g * LANES, (g + 1) * LANES)

    order = [row_peer(d) for d in sorted(range(rows), key=lambda d: -min(d, rows - d))]
    load_begins = [pltpu.make_async_copy(starts_ref.at[pl.ds(w, 1)], begins.at[w], bs.at[w]) for w in range(windows)]
    for c in load_begins:
        c.start()
    loads = [pltpu.make_async_copy(returns_ref.at[w], held.at[w], ls.at[w]) for w in order]
    for c in loads:
        c.start()
    load_firsts = pltpu.make_async_copy(start_ref.at[r], firsts, bs.at[windows])
    load_firsts.start()

    barrier = pltpu.get_barrier_semaphore()
    for d in range(1, rows):
        pl.semaphore_signal(barrier, inc=1, device_id=row_id(row_peer(d)), device_id_type=MESH)
    for d in range(1, mates):
        pl.semaphore_signal(barrier, inc=1, device_id=mate_id(mate(d)), device_id_type=MESH)

    def unit(s, w, q, sem=None):
        return pltpu.make_async_remote_copy(
            src_ref=codes.at[s, w], dst_ref=codes.at[s, w],
            send_sem=cs.at[w] if sem is None else sem.at[0], recv_sem=cr.at[s, w],
            device_id=row_id(q), device_id_type=MESH)

    def gain(s, q):
        return pltpu.make_async_remote_copy(
            src_ref=gains.at[s], dst_ref=gains.at[s], send_sem=gs.at[q],
            recv_sem=gr.at[s], device_id=row_id(q), device_id_type=MESH)

    row = lax.broadcasted_iota(jnp.int32, (groups, LANES), 0)
    own_day = r * days + lax.broadcasted_iota(jnp.int32, (days, LANES), 0)

    def encode(w):
        def load(g):
            x = held[w, :, lanes(g)]
            return jnp.where(own_day >= begins[w, :, lanes(g)], x, x[days - 1:days])

        centers = jnp.zeros((groups, LANES), jnp.float32)
        reach = jnp.full((1, LANES), TINY, jnp.float32)
        middles = []
        for g in range(groups):
            x = load(g)
            top = jnp.max(x, axis=0, keepdims=True)
            low = jnp.min(x, axis=0, keepdims=True)
            center = jnp.round((top + low) * (0.5 * TOP / LIMIT))
            middle = center * (LIMIT / TOP)
            reach = jnp.maximum(reach, jnp.maximum(top - middle, middle - low))
            centers = jnp.where(row == g, center, centers)
            middles.append(middle)
        codes[r, w, groups] = centers.astype(jnp.int32).astype(jnp.int16)
        gains[r, w] = reach * (1.0 / TOP)
        inverse = TOP / reach
        for g in range(groups):
            codes[r, w, g] = jnp.round((load(g) - middles[g]) * inverse).astype(jnp.int32).astype(jnp.int16)

    plans = [background(rows, windows, x) for x in range(rows)]

    def stage(number):
        for x, plan in enumerate(plans):
            some = [p for p in plan if p[3] == number]
            if some:
                @pl.when(r == x)
                def _():
                    for s, w, q, _ in some:
                        if number > 4:
                            unit(s, w, q).wait_recv()
                        unit(s, w, q, rest).start()

    def relayed(s, w):
        flags = [jnp.logical_and(r == near, jnp.logical_and(s != e, w != e)) for e, near in ends]
        return functools.reduce(jnp.logical_or, flags)

    for c in load_begins:
        c.wait()
    for i, w in enumerate(order):
        loads[i].wait()
        encode(w)
        if i == 1:
            pl.semaphore_wait(barrier, rows - 1 + mates - 1)
        if i > 0:
            unit(r, order[i - 1], order[i - 1]).start()
    for d in range(1, rows):
        gain(r, row_peer(d)).start()
    stage(0)

    load_firsts.wait()
    lhs[:k] = firsts[...].astype(jnp.bfloat16)
    for w in order[:-1]:
        unit(r, w, w).wait_send()
    for d in range(1, subs):
        pl.semaphore_signal(clear, inc=1, device_id={"sub": lax.rem(lax.axis_index("sub") + d, subs)},
                            device_id_type=MESH)
    pl.semaphore_wait(clear, subs - 1)
    stage(1)

    day = lax.broadcasted_iota(jnp.int32, (total, LANES), 0)

    def standardize(w, store):
        middles = [codes[s, w, groups].astype(jnp.float32) * (LIMIT / TOP) for s in range(rows)]
        steps = [gains[s, w] for s in range(rows)]
        for g in range(groups):
            x = jnp.concatenate([
                codes[s, w, g].astype(jnp.float32) * steps[s] + middles[s][g:g + 1]
                for s in range(rows)], axis=0)
            begin = begins[w, :, lanes(g)]
            live = day >= begin
            counts = (total - begin).astype(jnp.float32)
            mean = jnp.sum(jnp.where(live, x, 0.0), axis=0, keepdims=True) / counts
            centered = jnp.where(live, x - mean, 0.0)
            squares = jnp.sum(centered * centered, axis=0, keepdims=True)
            store(g, (centered * lax.rsqrt(squares + 1.0)).astype(jnp.bfloat16))

    for d in range(1, rows):
        gain(row_peer(d), r).wait_recv()
        unit(row_peer(d), r, r).wait_recv()
    stage(4)

    def keep_own(g, value):
        lhs[k:, lanes(g)] = value

    standardize(r, keep_own)
    sums = lax.dot_general(lhs[...], lhs[k:], NT, preferred_element_type=jnp.float32)
    summed = jnp.concatenate([sums[:half], sums[half:]], axis=1)
    mine[...] = summed
    sends = []
    for d in range(1, mates):
        q = mate(d)
        c = pltpu.make_async_remote_copy(
            src_ref=mine, dst_ref=quad.at[m], send_sem=qs.at[d], recv_sem=qr.at[m],
            device_id=mate_id(q), device_id_type=MESH)
        c.start()
        sends.append(c)
    quad[m] = summed
    stage(2)
    for d in range(1, mates):
        q = mate(d)
        pltpu.make_async_remote_copy(
            src_ref=mine, dst_ref=quad.at[q], send_sem=qs.at[d], recv_sem=qr.at[q],
            device_id=mate_id(q), device_id_type=MESH).wait_recv()
    stage(3)
    stage(5)
    both = quad[0]
    for q in range(1, mates):
        both = both + quad[q]
    both = jnp.concatenate([both[:, :total], both[:, total:]], axis=0)
    proj, corr = both[:k], both[k:]
    image = exact(proj, corr)
    for step in range(ITERS):
        gram = lax.dot_general(image, proj, NT, precision=HIGHEST,
                               preferred_element_type=jnp.float32) / assets
        if step < ITERS - 1:
            proj, image = eliminate(gram, [image, exact(image, corr)])
        else:
            proj, = eliminate(gram, [proj])
    high = proj.astype(jnp.bfloat16)
    low = (proj - high.astype(jnp.float32)).astype(jnp.bfloat16)
    mix[r] = jnp.concatenate([high, low], axis=0)

    def deliver(slot, q):
        return pltpu.make_async_remote_copy(
            src_ref=mix.at[slot], dst_ref=mix.at[slot], send_sem=ms.at[q], recv_sem=mr.at[slot],
            device_id=row_id(q), device_id_type=MESH)

    for q in order[:-1]:
        deliver(r, q).start()
    stage(6)

    def finish(w, scaled):
        wide = jnp.dot(mix[w], scaled, preferred_element_type=jnp.float32)
        out_ref[w] = wide[:k] + wide[k:]

    finish(r, lhs[k:])
    upper = r >= rows // 2
    mirrored = jnp.where(upper, r, rows - 1 - r)
    turn = []
    for j in range(rows - 1):
        inner = jnp.where(mirrored > j, j, j + 1)
        w = jnp.where(mirrored == rows - 1, rows - 2 if j == 0 else j - 1, inner)
        turn.append(jnp.where(upper, w, rows - 1 - w))
    for w in turn:
        for b in range(1, rows):
            s = row_peer(b)

            @pl.when(jnp.logical_not(relayed(s, w)))
            def _():
                unit(s, w, r).wait_recv()

        def keep(g, value):
            sbuf[w, :, lanes(g)] = value

        standardize(w, keep)
    for w in turn:
        deliver(w, w).wait_recv()
    for w in turn:
        finish(w, sbuf[w])
    for c in sends:
        c.wait_send()
    for d in range(1, rows):
        gain(r, row_peer(d)).wait_send()
    for q in order[:-1]:
        deliver(r, q).wait_send()
    for count in sorted({len(plan) for plan in plans}):
        high, wide = block(count, rows, windows)
        some = [x for x, plan in enumerate(plans) if len(plan) == count]

        @pl.when(functools.reduce(jnp.logical_or, [r == x for x in some]))
        def _():
            whole = codes.at[pl.ds(0, high), pl.ds(0, wide)]
            pltpu.make_async_remote_copy(
                src_ref=whole, dst_ref=whole, send_sem=rest.at[0], recv_sem=cr.at[0, 0],
                device_id=row_id(row_peer(1)), device_id_type=MESH).wait_send()


def fused(returns, starts, start_block, rows, cols, subs):
    windows, days, width = returns.shape
    k = start_block.shape[1]
    total = days * rows
    mates = cols * subs
    half = (k + total) // 2
    groups = width // LANES
    f32, bf16 = jnp.float32, jnp.bfloat16
    dma = pltpu.SemaphoreType.DMA
    return pl.pallas_call(
        functools.partial(kernel, rows, cols, subs, width * mates),
        out_shape=pltpu.VMEM(start_block.shape, f32),
        in_specs=[pl.BlockSpec(memory_space=pl.ANY)] * 3,
        out_specs=pl.BlockSpec(memory_space=pltpu.VMEM),
        scratch_shapes=[
            pltpu.VMEM(returns.shape, f32),
            pltpu.VMEM((windows, 1, width), jnp.int32),
            pltpu.VMEM((k, width), f32),
            pltpu.VMEM((rows, windows, groups + 1, days, LANES), jnp.int16),
            pltpu.VMEM((k + total, width), bf16),
            pltpu.VMEM((windows, total, width), bf16),
            pltpu.VMEM((half, 2 * total), f32),
            pltpu.VMEM((mates, half, 2 * total), f32),
            pltpu.VMEM((windows, 2 * k, total), bf16),
            pltpu.VMEM((rows, windows, 1, LANES), f32),
            dma((windows,)), dma((windows + 1,)),
            dma((windows,)), dma((rows, windows)),
            dma((mates,)), dma((mates,)),
            dma((rows,)), dma((rows,)), dma((rows,)), dma((rows,)), dma((1,)), pltpu.SemaphoreType.REGULAR,
        ],
        compiler_params=pltpu.CompilerParams(collective_id=0, has_side_effects=True),
    )(returns, starts, start_block)


def gram_of(image):
    return jnp.einsum("wkj,wlj->wkl", image, image, precision=HIGHEST)


def project(factors, scaled):
    rounded = factors.astype(jnp.bfloat16)
    return jnp.einsum("wka,wta->wkt", rounded, scaled, preferred_element_type=jnp.float32)


def expand(proj, widened):
    return jnp.einsum("wkt,wta->wka", proj, widened, precision=HIGHEST)


def orthonormal(image, gram, assets):
    lower = jnp.linalg.cholesky(gram / assets)
    return jax.scipy.linalg.solve_triangular(lower, image, lower=True)


def stepwise(returns, starts, start_block, rows, mates):
    windows, days, width = returns.shape
    row_pos = lax.axis_index("rows")
    total_days = days * rows
    day_index = row_pos * days + jnp.arange(days, dtype=jnp.int32)
    live = (day_index[None, :, None] >= starts[:, None, :]).astype(jnp.float32)
    counts = (total_days - starts).astype(jnp.float32)
    masked = live * returns
    sums = lax.psum(jnp.sum(masked, axis=1), "rows")
    mean = sums / counts
    centered = live * (returns - mean[:, None, :])
    squares = lax.psum(jnp.sum(centered * centered, axis=1), "rows")
    scaled = (centered * lax.rsqrt(squares + 1.0)[:, None, :]).astype(jnp.bfloat16)
    widened = scaled.astype(jnp.float32)
    factors = start_block
    for step in range(ITERS):
        proj = lax.psum(project(factors, scaled), ("cols", "sub"))
        image = lax.psum(expand(proj, widened), "rows")
        gram = lax.psum(gram_of(image), ("cols", "sub"))
        factors = orthonormal(image, gram, width * mates)
    return factors


def on_device(rows, cols, subs, returns, starts, start_block):
    windows, days, width = returns.shape
    k = start_block.shape[1]
    fits = (windows == rows and width == LANES * days and days % 16 == 0 and k % 16 == 0
            and days * rows <= 64 and (days * rows + k) % 16 == 0 and rows > 3 and cols * subs > 1
            and all(block(len(background(rows, windows, x)), rows, windows) for x in range(rows)))
    if fits:
        return fused(returns, starts, start_block, rows, cols, subs)
    return stepwise(returns, starts, start_block, rows, cols * subs)


def solution(mesh):
    placed = (
        P("groups", "rows", ("cols", "sub")),
        P("groups", ("cols", "sub")),
        P("groups", None, ("cols", "sub")),
    )
    sizes = (mesh.shape["rows"], mesh.shape["cols"], mesh.shape["sub"])
    return jax.shard_map(
        functools.partial(on_device, *sizes),
        mesh=mesh,
        in_specs=placed,
        out_specs=P("groups", None, ("cols", "sub")),
        check_vma=False,
    )
```

```python
import functools

import jax
import jax.numpy as jnp
from jax import lax
from jax.experimental import pallas as pl
from jax.experimental.pallas import tpu as pltpu
from jax.sharding import PartitionSpec as P

ITERS = 3
HIGHEST = lax.Precision.HIGHEST
MESH = pl.DeviceIdType.MESH
NT = (((1,), (1,)), ((), ()))
SUBLANES = 8
LANES = 128
LIMIT = 6.0
TOP = 32767.0
TINY = 1e-30
PIECES = 2


def eliminate(gram, rights):
    size, wide = gram.shape[0], rights[0].shape[1]
    tiles = size // SUBLANES
    sums = [[x[c * SUBLANES:(c + 1) * SUBLANES] for c in range(tiles)] for x in rights]
    row_id = lax.broadcasted_iota(jnp.int32, (SUBLANES, 1), 0)
    diag = [jnp.ones((SUBLANES, wide), jnp.float32) for _ in range(tiles)]
    panel = {
        (c, i): jnp.broadcast_to(gram[c * SUBLANES:(c + 1) * SUBLANES, i:i + 1], (SUBLANES, wide))
        for i in range(size) for c in range(i // SUBLANES, tiles)
    }
    for i in range(size):
        own, sub = i // SUBLANES, i % SUBLANES
        pivot = panel[own, i][sub:sub + 1]
        inverse = 1.0 / pivot
        diag[own] = jnp.where(row_id == sub, pivot, diag[own])
        ahead = {n: panel[n // SUBLANES, i][n % SUBLANES:n % SUBLANES + 1] for n in range(i + 1, size)}
        rows = [x[own][sub:sub + 1] for x in sums]
        for c in range(own, tiles):
            factor = panel[c, i] * inverse
            if c == own:
                factor = jnp.where(row_id > sub, factor, 0.0)
            for n in range(i + 1, size):
                if c >= n // SUBLANES:
                    panel[c, n] = panel[c, n] - factor * ahead[n]
            for x, row in zip(sums, rows):
                x[c] = x[c] - factor * row
    roots = [lax.rsqrt(d) for d in diag]
    return [jnp.concatenate([v * d for v, d in zip(x, roots)], axis=0) for x in sums]


def exact(left, right):
    return jnp.dot(left, right, precision=HIGHEST, preferred_element_type=jnp.float32)


def wanted(windows, x):
    some = [w for w in range(windows) if abs(w - x) > 1]
    return some if x >= windows // 2 else some[::-1]


def background(rows, windows, x):
    ends = (0, rows - 1)
    plan = []
    for q in range(rows):
        for d, w in enumerate(wanted(windows, q) if q != x else []):
            if abs(q - x) == 1:
                plan.append((w, q, 0 if q in ends or x in ends else 2))
            else:
                plan.append((w, q, 1 if q in ends and d == 0 else 2))
    return plan


def kernel(rows, cols, subs, assets,
           returns_ref, starts_ref, start_ref, out_ref,
           held, begins, firsts, codes, lhs, sbuf, mine, quad, mix, gains, made, got,
           ls, bs, cs, cr, qs, qr, ms, mr, gs, gr, rest, hs, hr, clear):
    r = lax.axis_index("rows")
    mates = cols * subs
    m = lax.axis_index("cols") * subs + lax.axis_index("sub")
    windows, days, width = returns_ref.shape
    k = start_ref.shape[1]
    total = days * rows
    groups = width // LANES
    half = (k + total) // 2
    def row_peer(d):
        return lax.rem(r + d, rows)

    def mate(d):
        return lax.rem(m + d, mates)

    def row_id(q):
        return {"rows": q}

    def mate_id(q):
        return {"cols": q // subs, "sub": lax.rem(q, subs)}

    def lanes(g):
        return slice(g * LANES, (g + 1) * LANES)

    order = [row_peer(d) for d in sorted(range(rows), key=lambda d: -min(d, rows - d))]
    load_begins = [pltpu.make_async_copy(starts_ref.at[pl.ds(w, 1)], begins.at[w], bs.at[w]) for w in range(windows)]
    for c in load_begins:
        c.start()
    loads = [pltpu.make_async_copy(returns_ref.at[w], held.at[w], ls.at[w]) for w in order]
    for c in loads:
        c.start()
    load_firsts = pltpu.make_async_copy(start_ref.at[r], firsts, bs.at[windows])
    load_firsts.start()

    barrier = pltpu.get_barrier_semaphore()
    for d in range(1, rows):
        pl.semaphore_signal(barrier, inc=1, device_id=row_id(row_peer(d)), device_id_type=MESH)
    for d in range(1, mates):
        pl.semaphore_signal(barrier, inc=1, device_id=mate_id(mate(d)), device_id_type=MESH)

    def unit(s, w, q, sem=None):
        return pltpu.make_async_remote_copy(
            src_ref=codes.at[s * windows + w], dst_ref=codes.at[s * windows + w],
            send_sem=cs.at[w] if sem is None else sem.at[0], recv_sem=cr.at[s, w],
            device_id=row_id(q), device_id_type=MESH)

    def gain(s, q):
        return pltpu.make_async_remote_copy(
            src_ref=gains.at[s], dst_ref=gains.at[s], send_sem=gs.at[q],
            recv_sem=gr.at[s], device_id=row_id(q), device_id_type=MESH)

    row = lax.broadcasted_iota(jnp.int32, (groups, LANES), 0)
    own_day = r * days + lax.broadcasted_iota(jnp.int32, (days, LANES), 0)

    def encode(w):
        def load(g):
            x = held[w, :, lanes(g)]
            return jnp.where(own_day >= begins[w, :, lanes(g)], x, x[days - 1:days])

        centers = jnp.zeros((groups, LANES), jnp.float32)
        reach = jnp.full((1, LANES), TINY, jnp.float32)
        middles = []
        for g in range(groups):
            x = load(g)
            top = jnp.max(x, axis=0, keepdims=True)
            low = jnp.min(x, axis=0, keepdims=True)
            center = jnp.round((top + low) * (0.5 * TOP / LIMIT))
            middle = center * (LIMIT / TOP)
            reach = jnp.maximum(reach, jnp.maximum(top - middle, middle - low))
            centers = jnp.where(row == g, center, centers)
            middles.append(middle)
        codes[r * windows + w, groups] = centers.astype(jnp.int32).astype(jnp.int16)
        gains[r, w] = reach * (1.0 / TOP)
        inverse = TOP / reach
        for g in range(groups):
            codes[r * windows + w, g] = jnp.round((load(g) - middles[g]) * inverse).astype(jnp.int32).astype(jnp.int16)

    plans = [background(rows, windows, x) for x in range(rows)]

    def per_row(act):
        for x in range(rows):
            @pl.when(r == x)
            def _():
                act(x)

    def stage(number):
        def act(x):
            for w, q, when in plans[x]:
                if when == number:
                    unit(x, w, q, rest).start()

        per_row(act)

    for c in load_begins:
        c.wait()
    for i, w in enumerate(order):
        loads[i].wait()
        encode(w)
        if i == 1:
            pl.semaphore_wait(barrier, rows - 1 + mates - 1)
        if i > 0:
            unit(r, order[i - 1], order[i - 1]).start()
    for d in range(1, rows):
        gain(r, row_peer(d)).start()
    stage(0)

    load_firsts.wait()
    lhs[:k] = firsts[...].astype(jnp.bfloat16)
    for w in order[:-1]:
        unit(r, w, w).wait_send()
    for d in range(1, subs):
        pl.semaphore_signal(clear, inc=1, device_id={"sub": lax.rem(lax.axis_index("sub") + d, subs)},
                            device_id_type=MESH)
    pl.semaphore_wait(clear, subs - 1)
    stage(1)

    day = lax.broadcasted_iota(jnp.int32, (total, LANES), 0)

    def standardize(w, store):
        middles = [codes[s * windows + w, groups].astype(jnp.float32) * (LIMIT / TOP) for s in range(rows)]
        steps = [gains[s, w] for s in range(rows)]
        for g in range(groups):
            x = jnp.concatenate([
                codes[s * windows + w, g].astype(jnp.float32) * steps[s] + middles[s][g:g + 1]
                for s in range(rows)], axis=0)
            begin = begins[w, :, lanes(g)]
            live = day >= begin
            counts = (total - begin).astype(jnp.float32)
            mean = jnp.sum(jnp.where(live, x, 0.0), axis=0, keepdims=True) / counts
            centered = jnp.where(live, x - mean, 0.0)
            squares = jnp.sum(centered * centered, axis=0, keepdims=True)
            store(g, (centered * lax.rsqrt(squares + 1.0)).astype(jnp.bfloat16))

    for d in range(1, rows):
        gain(row_peer(d), r).wait_recv()
        unit(row_peer(d), r, r).wait_recv()
    def keep_own(g, value):
        lhs[k:, lanes(g)] = value

    standardize(r, keep_own)
    sums = lax.dot_general(lhs[...], lhs[k:], NT, preferred_element_type=jnp.float32)
    summed = jnp.concatenate([sums[:half], sums[half:]], axis=1)
    mine[...] = summed
    sends = []
    for d in range(1, mates):
        q = mate(d)
        c = pltpu.make_async_remote_copy(
            src_ref=mine, dst_ref=quad.at[m], send_sem=qs.at[d], recv_sem=qr.at[m],
            device_id=mate_id(q), device_id_type=MESH)
        c.start()
        sends.append(c)
    quad[m] = summed
    stage(2)
    for d in range(1, mates):
        q = mate(d)
        pltpu.make_async_remote_copy(
            src_ref=mine, dst_ref=quad.at[q], send_sem=qs.at[d], recv_sem=qr.at[q],
            device_id=mate_id(q), device_id_type=MESH).wait_recv()
    both = quad[0]
    for q in range(1, mates):
        both = both + quad[q]
    both = jnp.concatenate([both[:, :total], both[:, total:]], axis=0)
    proj, corr = both[:k], both[k:]
    image = exact(proj, corr)
    for step in range(ITERS):
        gram = lax.dot_general(image, proj, NT, precision=HIGHEST,
                               preferred_element_type=jnp.float32) / assets
        if step < ITERS - 1:
            proj, image = eliminate(gram, [image, exact(image, corr)])
        else:
            proj, = eliminate(gram, [proj])
    high = proj.astype(jnp.bfloat16)
    low = (proj - high.astype(jnp.float32)).astype(jnp.bfloat16)
    mix[r] = jnp.concatenate([high, low], axis=0)

    def deliver(slot, q):
        return pltpu.make_async_remote_copy(
            src_ref=mix.at[slot], dst_ref=mix.at[slot], send_sem=ms.at[q], recv_sem=mr.at[slot],
            device_id=row_id(q), device_id_type=MESH)

    def spread(x):
        for q in range(rows):
            if abs(q - x) > 1:
                deliver(x, q).start()

    per_row(spread)

    def loadings(w, scaled):
        wide = jnp.dot(mix[w], scaled, preferred_element_type=jnp.float32)
        return (wide[:k] + wide[k:]).astype(jnp.bfloat16)

    part = width // PIECES

    def hand(h, side):
        return pltpu.make_async_remote_copy(
            src_ref=made.at[h], dst_ref=got.at[side, h], send_sem=hs.at[side, h], recv_sem=hr.at[side, h],
            device_id=row_id(r + 1 - 2 * side), device_id_type=MESH)

    def beside(act):
        for side in (0, 1):
            @pl.when(r < rows - 1 if side == 0 else r > 0)
            def _():
                act(side)

    for h in range(PIECES):
        some = slice(h * part, (h + 1) * part)
        value = loadings(r, lhs[k:, some])
        made[h] = value
        beside(lambda side: hand(h, side).start())
        out_ref[r, :, some] = value.astype(jnp.float32)

    lists = [wanted(windows, x) for x in range(rows)]
    most = max(len(v) for v in lists)
    for act in ("scale", "expand"):
        for j in range(most):
            have = [x for x in range(rows) if len(lists[x]) > j]
            w = sum(jnp.where(r == x, lists[x][j], 0) for x in have)

            @pl.when(functools.reduce(jnp.logical_or, [r == x for x in have]))
            def _():
                if act == "expand":
                    deliver(w, w).wait_recv()
                    out_ref[w] = loadings(w, sbuf[j]).astype(jnp.float32)
                    return

                for d in range(1, rows):
                    unit(row_peer(d), w, r).wait_recv()

                def keep(g, value):
                    sbuf[j, :, lanes(g)] = value

                standardize(w, keep)

    def collect(side):
        for h in range(PIECES):
            hand(h, side).wait_recv()
            out_ref[r - 1 + 2 * side, :, h * part:(h + 1) * part] = got[side, h].astype(jnp.float32)

    for side in (0, 1):
        @pl.when(r > 0 if side == 0 else r < rows - 1)
        def _():
            collect(side)

    for c in sends:
        c.wait_send()
    for d in range(1, rows):
        gain(r, row_peer(d)).wait_send()

    def settle(x):
        for q in range(rows):
            if abs(q - x) > 1:
                deliver(x, q).wait_send()
        if plans[x]:
            whole = codes.at[pl.ds(0, len(plans[x]))]
            pltpu.make_async_remote_copy(
                src_ref=whole, dst_ref=whole, send_sem=rest.at[0], recv_sem=cr.at[0, 0],
                device_id=row_id(row_peer(1)), device_id_type=MESH).wait_send()

    per_row(settle)
    for h in range(PIECES):
        beside(lambda side: hand(h, side).wait_send())


def fused(returns, starts, start_block, rows, cols, subs):
    windows, days, width = returns.shape
    k = start_block.shape[1]
    total = days * rows
    mates = cols * subs
    half = (k + total) // 2
    groups = width // LANES
    f32, bf16 = jnp.float32, jnp.bfloat16
    dma = pltpu.SemaphoreType.DMA
    return pl.pallas_call(
        functools.partial(kernel, rows, cols, subs, width * mates),
        out_shape=pltpu.VMEM(start_block.shape, f32),
        in_specs=[pl.BlockSpec(memory_space=pl.ANY)] * 3,
        out_specs=pl.BlockSpec(memory_space=pltpu.VMEM),
        scratch_shapes=[
            pltpu.VMEM(returns.shape, f32),
            pltpu.VMEM((windows, 1, width), jnp.int32),
            pltpu.VMEM((k, width), f32),
            pltpu.VMEM((rows * windows, groups + 1, days, LANES), jnp.int16),
            pltpu.VMEM((k + total, width), bf16),
            pltpu.VMEM((windows - 2, total, width), bf16),
            pltpu.VMEM((half, 2 * total), f32),
            pltpu.VMEM((mates, half, 2 * total), f32),
            pltpu.VMEM((windows, 2 * k, total), bf16),
            pltpu.VMEM((rows, windows, 1, LANES), f32),
            pltpu.VMEM((PIECES, k, width // PIECES), bf16),
            pltpu.VMEM((2, PIECES, k, width // PIECES), bf16),
            dma((windows,)), dma((windows + 1,)),
            dma((windows,)), dma((rows, windows)),
            dma((mates,)), dma((mates,)),
            dma((rows,)), dma((rows,)), dma((rows,)), dma((rows,)), dma((1,)), dma((2, PIECES)), dma((2, PIECES)), pltpu.SemaphoreType.REGULAR,
        ],
        compiler_params=pltpu.CompilerParams(collective_id=0, has_side_effects=True),
    )(returns, starts, start_block)


def gram_of(image):
    return jnp.einsum("wkj,wlj->wkl", image, image, precision=HIGHEST)


def project(factors, scaled):
    rounded = factors.astype(jnp.bfloat16)
    return jnp.einsum("wka,wta->wkt", rounded, scaled, preferred_element_type=jnp.float32)


def expand(proj, widened):
    return jnp.einsum("wkt,wta->wka", proj, widened, precision=HIGHEST)


def orthonormal(image, gram, assets):
    lower = jnp.linalg.cholesky(gram / assets)
    return jax.scipy.linalg.solve_triangular(lower, image, lower=True)


def stepwise(returns, starts, start_block, rows, mates):
    windows, days, width = returns.shape
    row_pos = lax.axis_index("rows")
    total_days = days * rows
    day_index = row_pos * days + jnp.arange(days, dtype=jnp.int32)
    live = (day_index[None, :, None] >= starts[:, None, :]).astype(jnp.float32)
    counts = (total_days - starts).astype(jnp.float32)
    masked = live * returns
    sums = lax.psum(jnp.sum(masked, axis=1), "rows")
    mean = sums / counts
    centered = live * (returns - mean[:, None, :])
    squares = lax.psum(jnp.sum(centered * centered, axis=1), "rows")
    scaled = (centered * lax.rsqrt(squares + 1.0)[:, None, :]).astype(jnp.bfloat16)
    widened = scaled.astype(jnp.float32)
    factors = start_block
    for step in range(ITERS):
        proj = lax.psum(project(factors, scaled), ("cols", "sub"))
        image = lax.psum(expand(proj, widened), "rows")
        gram = lax.psum(gram_of(image), ("cols", "sub"))
        factors = orthonormal(image, gram, width * mates)
    return factors


def on_device(rows, cols, subs, returns, starts, start_block):
    windows, days, width = returns.shape
    k = start_block.shape[1]
    fits = (windows == rows and width == LANES * days and days % 16 == 0 and k % 16 == 0
            and days * rows <= 64 and (days * rows + k) % 16 == 0 and rows == 4 and cols * subs > 1)
    if fits:
        return fused(returns, starts, start_block, rows, cols, subs)
    return stepwise(returns, starts, start_block, rows, cols * subs)


def solution(mesh):
    placed = (
        P("groups", "rows", ("cols", "sub")),
        P("groups", ("cols", "sub")),
        P("groups", None, ("cols", "sub")),
    )
    sizes = (mesh.shape["rows"], mesh.shape["cols"], mesh.shape["sub"])
    return jax.shard_map(
        functools.partial(on_device, *sizes),
        mesh=mesh,
        in_specs=placed,
        out_specs=P("groups", None, ("cols", "sub")),
        check_vma=False,
    )
```

```python
import functools

import jax
import jax.numpy as jnp
from jax import lax
from jax.experimental import pallas as pl
from jax.experimental.pallas import tpu as pltpu
from jax.sharding import PartitionSpec as P

ITERS = 3
HIGHEST = lax.Precision.HIGHEST
MESH = pl.DeviceIdType.MESH
NT = (((1,), (1,)), ((), ()))
SUBLANES = 8
LANES = 128
LIMIT = 6.0
TOP = 32767.0
TINY = 1e-30
PIECES = 2


def eliminate(gram, rights):
    size, wide = gram.shape[0], rights[0].shape[1]
    tiles = size // SUBLANES
    sums = [[x[c * SUBLANES:(c + 1) * SUBLANES] for c in range(tiles)] for x in rights]
    row_id = lax.broadcasted_iota(jnp.int32, (SUBLANES, 1), 0)
    diag = [jnp.ones((SUBLANES, wide), jnp.float32) for _ in range(tiles)]
    panel = {
        (c, i): jnp.broadcast_to(gram[c * SUBLANES:(c + 1) * SUBLANES, i:i + 1], (SUBLANES, wide))
        for i in range(size) for c in range(i // SUBLANES, tiles)
    }
    for i in range(size):
        own, sub = i // SUBLANES, i % SUBLANES
        pivot = panel[own, i][sub:sub + 1]
        inverse = 1.0 / pivot
        diag[own] = jnp.where(row_id == sub, pivot, diag[own])
        ahead = {n: panel[n // SUBLANES, i][n % SUBLANES:n % SUBLANES + 1] for n in range(i + 1, size)}
        rows = [x[own][sub:sub + 1] for x in sums]
        for c in range(own, tiles):
            factor = panel[c, i] * inverse
            if c == own:
                factor = jnp.where(row_id > sub, factor, 0.0)
            for n in range(i + 1, size):
                if c >= n // SUBLANES:
                    panel[c, n] = panel[c, n] - factor * ahead[n]
            for x, row in zip(sums, rows):
                x[c] = x[c] - factor * row
    roots = [lax.rsqrt(d) for d in diag]
    return [jnp.concatenate([v * d for v, d in zip(x, roots)], axis=0) for x in sums]


def exact(left, right):
    return jnp.dot(left, right, precision=HIGHEST, preferred_element_type=jnp.float32)


def wanted(windows, x):
    some = [w for w in range(windows) if w != x and (abs(w - x) > 1 or w in (0, windows - 1))]
    return some if x >= windows // 2 else some[::-1]


def background(rows, windows, x):
    ends = (0, rows - 1)
    plan = []
    for q in range(rows):
        for w in wanted(windows, q) if q != x else []:
            if q in ends:
                plan.append((x, w, q, 0 if abs(q - x) == 1 else 1))
            elif x in ends and abs(q - x) == 1:
                plan.append((x, w, q, 2 if w == x else 0))
            elif abs(q - x) == 1 and abs(w - q) > 1:
                plan.append((x, w, q, 1))
    if x in ends:
        near = 1 if x == 0 else rows - 2
        for s in range(rows):
            if s not in (x, near):
                plan.append((s, x, near, 2))
                plan += [(s, w, near, 3) for w in wanted(windows, near) if w == s]
    return plan


def kernel(rows, cols, subs, assets,
           returns_ref, starts_ref, start_ref, out_ref,
           held, begins, firsts, codes, lhs, sbuf, mine, quad, mix, gains, made, got,
           ls, bs, cs, cr, qs, qr, ms, mr, gs, gr, rest, hs, hr, clear):
    r = lax.axis_index("rows")
    mates = cols * subs
    m = lax.axis_index("cols") * subs + lax.axis_index("sub")
    windows, days, width = returns_ref.shape
    k = start_ref.shape[1]
    total = days * rows
    groups = width // LANES
    half = (k + total) // 2
    def row_peer(d):
        return lax.rem(r + d, rows)

    def mate(d):
        return lax.rem(m + d, mates)

    def row_id(q):
        return {"rows": q}

    def mate_id(q):
        return {"cols": q // subs, "sub": lax.rem(q, subs)}

    def lanes(g):
        return slice(g * LANES, (g + 1) * LANES)

    order = [row_peer(d) for d in sorted(range(rows), key=lambda d: -min(d, rows - d))]
    load_begins = [pltpu.make_async_copy(starts_ref.at[pl.ds(w, 1)], begins.at[w], bs.at[w]) for w in range(windows)]
    for c in load_begins:
        c.start()
    loads = [pltpu.make_async_copy(returns_ref.at[w], held.at[w], ls.at[w]) for w in order]
    for c in loads:
        c.start()
    load_firsts = pltpu.make_async_copy(start_ref.at[r], firsts, bs.at[windows])
    load_firsts.start()

    barrier = pltpu.get_barrier_semaphore()
    for d in range(1, rows):
        pl.semaphore_signal(barrier, inc=1, device_id=row_id(row_peer(d)), device_id_type=MESH)
    for d in range(1, mates):
        pl.semaphore_signal(barrier, inc=1, device_id=mate_id(mate(d)), device_id_type=MESH)

    def unit(s, w, q, sem=None):
        return pltpu.make_async_remote_copy(
            src_ref=codes.at[s * windows + w], dst_ref=codes.at[s * windows + w],
            send_sem=cs.at[w] if sem is None else sem.at[0], recv_sem=cr.at[s, w],
            device_id=row_id(q), device_id_type=MESH)

    def gain(s, q):
        return pltpu.make_async_remote_copy(
            src_ref=gains.at[s], dst_ref=gains.at[s], send_sem=gs.at[q],
            recv_sem=gr.at[s], device_id=row_id(q), device_id_type=MESH)

    row = lax.broadcasted_iota(jnp.int32, (groups, LANES), 0)
    own_day = r * days + lax.broadcasted_iota(jnp.int32, (days, LANES), 0)

    def encode(w):
        def load(g):
            x = held[w, :, lanes(g)]
            return jnp.where(own_day >= begins[w, :, lanes(g)], x, x[days - 1:days])

        centers = jnp.zeros((groups, LANES), jnp.float32)
        reach = jnp.full((1, LANES), TINY, jnp.float32)
        middles = []
        for g in range(groups):
            x = load(g)
            top = jnp.max(x, axis=0, keepdims=True)
            low = jnp.min(x, axis=0, keepdims=True)
            center = jnp.round((top + low) * (0.5 * TOP / LIMIT))
            middle = center * (LIMIT / TOP)
            reach = jnp.maximum(reach, jnp.maximum(top - middle, middle - low))
            centers = jnp.where(row == g, center, centers)
            middles.append(middle)
        codes[r * windows + w, groups] = centers.astype(jnp.int32).astype(jnp.int16)
        gains[r, w] = reach * (1.0 / TOP)
        inverse = TOP / reach
        for g in range(groups):
            codes[r * windows + w, g] = jnp.round((load(g) - middles[g]) * inverse).astype(jnp.int32).astype(jnp.int16)

    plans = [background(rows, windows, x) for x in range(rows)]

    def per_row(act):
        for x in range(rows):
            @pl.when(r == x)
            def _():
                act(x)

    def stage(number):
        def act(x):
            for s, w, q, when in plans[x]:
                if when == number:
                    if s != x and w != x:
                        unit(s, w, q).wait_recv()
                    unit(s, w, q, rest).start()

        per_row(act)

    for c in load_begins:
        c.wait()
    for i, w in enumerate(order):
        loads[i].wait()
        encode(w)
        if i == 1:
            pl.semaphore_wait(barrier, rows - 1 + mates - 1)
        if i > 0:
            unit(r, order[i - 1], order[i - 1]).start()
    for d in range(1, rows):
        gain(r, row_peer(d)).start()
    stage(0)

    load_firsts.wait()
    lhs[:k] = firsts[...].astype(jnp.bfloat16)
    for w in order[:-1]:
        unit(r, w, w).wait_send()
    for d in range(1, subs):
        pl.semaphore_signal(clear, inc=1, device_id={"sub": lax.rem(lax.axis_index("sub") + d, subs)},
                            device_id_type=MESH)
    pl.semaphore_wait(clear, subs - 1)
    stage(1)

    day = lax.broadcasted_iota(jnp.int32, (total, LANES), 0)

    def standardize(w, store):
        middles = [codes[s * windows + w, groups].astype(jnp.float32) * (LIMIT / TOP) for s in range(rows)]
        steps = [gains[s, w] for s in range(rows)]
        for g in range(groups):
            x = jnp.concatenate([
                codes[s * windows + w, g].astype(jnp.float32) * steps[s] + middles[s][g:g + 1]
                for s in range(rows)], axis=0)
            begin = begins[w, :, lanes(g)]
            live = day >= begin
            counts = (total - begin).astype(jnp.float32)
            mean = jnp.sum(jnp.where(live, x, 0.0), axis=0, keepdims=True) / counts
            centered = jnp.where(live, x - mean, 0.0)
            squares = jnp.sum(centered * centered, axis=0, keepdims=True)
            store(g, (centered * lax.rsqrt(squares + 1.0)).astype(jnp.bfloat16))

    for d in range(1, rows):
        gain(row_peer(d), r).wait_recv()
        unit(row_peer(d), r, r).wait_recv()
    def keep_own(g, value):
        lhs[k:, lanes(g)] = value

    standardize(r, keep_own)
    sums = lax.dot_general(lhs[...], lhs[k:], NT, preferred_element_type=jnp.float32)
    summed = jnp.concatenate([sums[:half], sums[half:]], axis=1)
    mine[...] = summed
    sends = []
    for d in range(1, mates):
        q = mate(d)
        c = pltpu.make_async_remote_copy(
            src_ref=mine, dst_ref=quad.at[m], send_sem=qs.at[d], recv_sem=qr.at[m],
            device_id=mate_id(q), device_id_type=MESH)
        c.start()
        sends.append(c)
    quad[m] = summed
    stage(2)
    for d in range(1, mates):
        q = mate(d)
        pltpu.make_async_remote_copy(
            src_ref=mine, dst_ref=quad.at[q], send_sem=qs.at[d], recv_sem=qr.at[q],
            device_id=mate_id(q), device_id_type=MESH).wait_recv()
    both = quad[0]
    for q in range(1, mates):
        both = both + quad[q]
    both = jnp.concatenate([both[:, :total], both[:, total:]], axis=0)
    proj, corr = both[:k], both[k:]
    image = exact(proj, corr)
    for step in range(ITERS):
        gram = lax.dot_general(image, proj, NT, precision=HIGHEST,
                               preferred_element_type=jnp.float32) / assets
        if step < ITERS - 1:
            proj, image = eliminate(gram, [image, exact(image, corr)])
        else:
            proj, = eliminate(gram, [proj])
    high = proj.astype(jnp.bfloat16)
    low = (proj - high.astype(jnp.float32)).astype(jnp.bfloat16)
    mix[r] = jnp.concatenate([high, low], axis=0)

    def deliver(slot, q):
        return pltpu.make_async_remote_copy(
            src_ref=mix.at[slot], dst_ref=mix.at[slot], send_sem=ms.at[q], recv_sem=mr.at[slot],
            device_id=row_id(q), device_id_type=MESH)

    def spread(x):
        for q in range(rows):
            if x in wanted(windows, q):
                deliver(x, q).start()

    per_row(spread)
    stage(3)

    def loadings(w, scaled):
        wide = jnp.dot(mix[w], scaled, preferred_element_type=jnp.float32)
        return (wide[:k] + wide[k:]).astype(jnp.bfloat16)

    part = width // PIECES

    def hand(h, side):
        return pltpu.make_async_remote_copy(
            src_ref=made.at[h], dst_ref=got.at[side, h], send_sem=hs.at[side, h], recv_sem=hr.at[side, h],
            device_id=row_id(r + 1 - 2 * side), device_id_type=MESH)

    def inner(row):
        return jnp.logical_and(row > 0, row < rows - 1)

    for h in range(PIECES):
        some = slice(h * part, (h + 1) * part)
        value = loadings(r, lhs[k:, some])
        made[h] = value

        @pl.when(inner(r))
        def _():
            for side in (0, 1):
                hand(h, side).start()

        out_ref[r, :, some] = value.astype(jnp.float32)

    lists = [wanted(windows, x) for x in range(rows)]
    most = max(len(v) for v in lists)
    for act in ("scale", "expand"):
        for j in range(most):
            have = [x for x in range(rows) if len(lists[x]) > j]
            w = sum(jnp.where(r == x, lists[x][j], 0) for x in have)

            @pl.when(functools.reduce(jnp.logical_or, [r == x for x in have]))
            def _():
                if act == "expand":
                    deliver(w, w).wait_recv()
                    out_ref[w] = loadings(w, sbuf[j]).astype(jnp.float32)
                    return

                for d in range(1, rows):
                    s = row_peer(d)

                    @pl.when(jnp.logical_not(functools.reduce(jnp.logical_or, [
                        jnp.logical_and(r == x, jnp.logical_and(s == p[0], w == p[1]))
                        for x in range(rows) for p in plans[x] if p[0] != x and p[1] != x])))
                    def _():
                        unit(s, w, r).wait_recv()

                def keep(g, value):
                    sbuf[j, :, lanes(g)] = value

                standardize(w, keep)

    def collect(side):
        for h in range(PIECES):
            hand(h, side).wait_recv()
            out_ref[r - 1 + 2 * side, :, h * part:(h + 1) * part] = got[side, h].astype(jnp.float32)

    for side in (0, 1):
        @pl.when(inner(r - 1 + 2 * side))
        def _():
            collect(side)

    for c in sends:
        c.wait_send()
    for d in range(1, rows):
        gain(r, row_peer(d)).wait_send()

    def settle(x):
        for q in range(rows):
            if x in wanted(windows, q):
                deliver(x, q).wait_send()
        if plans[x]:
            whole = codes.at[pl.ds(0, len(plans[x]))]
            pltpu.make_async_remote_copy(
                src_ref=whole, dst_ref=whole, send_sem=rest.at[0], recv_sem=cr.at[0, 0],
                device_id=row_id(row_peer(1)), device_id_type=MESH).wait_send()

    per_row(settle)
    @pl.when(inner(r))
    def _():
        for h in range(PIECES):
            for side in (0, 1):
                hand(h, side).wait_send()


def fused(returns, starts, start_block, rows, cols, subs):
    windows, days, width = returns.shape
    k = start_block.shape[1]
    total = days * rows
    mates = cols * subs
    half = (k + total) // 2
    groups = width // LANES
    f32, bf16 = jnp.float32, jnp.bfloat16
    dma = pltpu.SemaphoreType.DMA
    return pl.pallas_call(
        functools.partial(kernel, rows, cols, subs, width * mates),
        out_shape=pltpu.VMEM(start_block.shape, f32),
        in_specs=[pl.BlockSpec(memory_space=pl.ANY)] * 3,
        out_specs=pl.BlockSpec(memory_space=pltpu.VMEM),
        scratch_shapes=[
            pltpu.VMEM(returns.shape, f32),
            pltpu.VMEM((windows, 1, width), jnp.int32),
            pltpu.VMEM((k, width), f32),
            pltpu.VMEM((rows * windows, groups + 1, days, LANES), jnp.int16),
            pltpu.VMEM((k + total, width), bf16),
            pltpu.VMEM((windows - 2, total, width), bf16),
            pltpu.VMEM((half, 2 * total), f32),
            pltpu.VMEM((mates, half, 2 * total), f32),
            pltpu.VMEM((windows, 2 * k, total), bf16),
            pltpu.VMEM((rows, windows, 1, LANES), f32),
            pltpu.VMEM((PIECES, k, width // PIECES), bf16),
            pltpu.VMEM((2, PIECES, k, width // PIECES), bf16),
            dma((windows,)), dma((windows + 1,)),
            dma((windows,)), dma((rows, windows)),
            dma((mates,)), dma((mates,)),
            dma((rows,)), dma((rows,)), dma((rows,)), dma((rows,)), dma((1,)), dma((2, PIECES)), dma((2, PIECES)), pltpu.SemaphoreType.REGULAR,
        ],
        compiler_params=pltpu.CompilerParams(collective_id=0, has_side_effects=True),
    )(returns, starts, start_block)


def gram_of(image):
    return jnp.einsum("wkj,wlj->wkl", image, image, precision=HIGHEST)


def project(factors, scaled):
    rounded = factors.astype(jnp.bfloat16)
    return jnp.einsum("wka,wta->wkt", rounded, scaled, preferred_element_type=jnp.float32)


def expand(proj, widened):
    return jnp.einsum("wkt,wta->wka", proj, widened, precision=HIGHEST)


def orthonormal(image, gram, assets):
    lower = jnp.linalg.cholesky(gram / assets)
    return jax.scipy.linalg.solve_triangular(lower, image, lower=True)


def stepwise(returns, starts, start_block, rows, mates):
    windows, days, width = returns.shape
    row_pos = lax.axis_index("rows")
    total_days = days * rows
    day_index = row_pos * days + jnp.arange(days, dtype=jnp.int32)
    live = (day_index[None, :, None] >= starts[:, None, :]).astype(jnp.float32)
    counts = (total_days - starts).astype(jnp.float32)
    masked = live * returns
    sums = lax.psum(jnp.sum(masked, axis=1), "rows")
    mean = sums / counts
    centered = live * (returns - mean[:, None, :])
    squares = lax.psum(jnp.sum(centered * centered, axis=1), "rows")
    scaled = (centered * lax.rsqrt(squares + 1.0)[:, None, :]).astype(jnp.bfloat16)
    widened = scaled.astype(jnp.float32)
    factors = start_block
    for step in range(ITERS):
        proj = lax.psum(project(factors, scaled), ("cols", "sub"))
        image = lax.psum(expand(proj, widened), "rows")
        gram = lax.psum(gram_of(image), ("cols", "sub"))
        factors = orthonormal(image, gram, width * mates)
    return factors


def on_device(rows, cols, subs, returns, starts, start_block):
    windows, days, width = returns.shape
    k = start_block.shape[1]
    fits = (windows == rows and width == LANES * days and days % 16 == 0 and k % 16 == 0
            and days * rows <= 64 and (days * rows + k) % 16 == 0 and rows == 4 and cols * subs > 1)
    if fits:
        return fused(returns, starts, start_block, rows, cols, subs)
    return stepwise(returns, starts, start_block, rows, cols * subs)


def solution(mesh):
    placed = (
        P("groups", "rows", ("cols", "sub")),
        P("groups", ("cols", "sub")),
        P("groups", None, ("cols", "sub")),
    )
    sizes = (mesh.shape["rows"], mesh.shape["cols"], mesh.shape["sub"])
    return jax.shard_map(
        functools.partial(on_device, *sizes),
        mesh=mesh,
        in_specs=placed,
        out_specs=P("groups", None, ("cols", "sub")),
        check_vma=False,
    )
```

```python
import functools

import jax
import jax.numpy as jnp
from jax import lax
from jax.experimental import pallas as pl
from jax.experimental.pallas import tpu as pltpu
from jax.sharding import PartitionSpec as P

ITERS = 3
HIGHEST = lax.Precision.HIGHEST
MESH = pl.DeviceIdType.MESH
NT = (((1,), (1,)), ((), ()))
SUBLANES = 8
LANES = 128
LIMIT = 6.0
TOP = 32767.0
TINY = 1e-30
PIECES = 2


def eliminate(gram, rights):
    size, wide = gram.shape[0], rights[0].shape[1]
    tiles = size // SUBLANES
    sums = [[x[c * SUBLANES:(c + 1) * SUBLANES] for c in range(tiles)] for x in rights]
    row_id = lax.broadcasted_iota(jnp.int32, (SUBLANES, 1), 0)
    diag = [jnp.ones((SUBLANES, wide), jnp.float32) for _ in range(tiles)]
    panel = {
        (c, i): jnp.broadcast_to(gram[c * SUBLANES:(c + 1) * SUBLANES, i:i + 1], (SUBLANES, wide))
        for i in range(size) for c in range(i // SUBLANES, tiles)
    }
    for i in range(size):
        own, sub = i // SUBLANES, i % SUBLANES
        pivot = panel[own, i][sub:sub + 1]
        inverse = 1.0 / pivot
        diag[own] = jnp.where(row_id == sub, pivot, diag[own])
        ahead = {n: panel[n // SUBLANES, i][n % SUBLANES:n % SUBLANES + 1] for n in range(i + 1, size)}
        rows = [x[own][sub:sub + 1] for x in sums]
        for c in range(own, tiles):
            factor = panel[c, i] * inverse
            if c == own:
                factor = jnp.where(row_id > sub, factor, 0.0)
            for n in range(i + 1, size):
                if c >= n // SUBLANES:
                    panel[c, n] = panel[c, n] - factor * ahead[n]
            for x, row in zip(sums, rows):
                x[c] = x[c] - factor * row
    roots = [lax.rsqrt(d) for d in diag]
    return [jnp.concatenate([v * d for v, d in zip(x, roots)], axis=0) for x in sums]


def exact(left, right):
    return jnp.dot(left, right, precision=HIGHEST, preferred_element_type=jnp.float32)


def wanted(windows, x):
    some = [w for w in range(windows) if w != x and (abs(w - x) > 1 or w in (0, windows - 1))]
    return some if x >= windows // 2 else some[::-1]


def background(rows, windows, x):
    ends = (0, rows - 1)
    plan = []
    for q in range(rows):
        for w in wanted(windows, q) if q != x else []:
            if q in ends:
                plan.append((x, w, q, 0 if abs(q - x) == 1 else 1))
            elif x in ends and abs(q - x) == 1:
                plan.append((x, w, q, 2 if w == x else 0))
            elif abs(q - x) == 1 and abs(w - q) > 1:
                plan.append((x, w, q, 1))
    if x in ends:
        near = 1 if x == 0 else rows - 2
        for s in range(rows):
            if s not in (x, near):
                plan.append((s, x, near, 2))
                plan += [(s, w, near, 3) for w in wanted(windows, near) if w == s]
    return plan


def kernel(rows, cols, subs, assets,
           returns_ref, starts_ref, start_ref, out_ref,
           held, begins, firsts, codes, lhs, sbuf, mine, quad, mix, gains, made, got,
           ls, bs, cs, pr, cr, rr, qs, qr, ms, mr, gs, gr, rest, hs, hr, clear):
    r = lax.axis_index("rows")
    mates = cols * subs
    m = lax.axis_index("cols") * subs + lax.axis_index("sub")
    windows, days, width = returns_ref.shape
    k = start_ref.shape[1]
    total = days * rows
    groups = width // LANES
    half = (k + total) // 2
    def row_peer(d):
        return lax.rem(r + d, rows)

    def mate(d):
        return lax.rem(m + d, mates)

    def row_id(q):
        return {"rows": q}

    def mate_id(q):
        return {"cols": q // subs, "sub": lax.rem(q, subs)}

    def lanes(g):
        return slice(g * LANES, (g + 1) * LANES)

    order = [row_peer(d) for d in sorted(range(rows), key=lambda d: -min(d, rows - d))]
    load_begins = [pltpu.make_async_copy(starts_ref.at[pl.ds(w, 1)], begins.at[w], bs.at[0]) for w in range(windows)]
    for c in load_begins:
        c.start()
    loads = [pltpu.make_async_copy(returns_ref.at[w], held.at[w], ls.at[w]) for w in order]
    for c in loads:
        c.start()
    load_firsts = pltpu.make_async_copy(start_ref.at[r], firsts, bs.at[1])
    load_firsts.start()

    barrier = pltpu.get_barrier_semaphore()
    for d in range(1, rows):
        pl.semaphore_signal(barrier, inc=1, device_id=row_id(row_peer(d)), device_id_type=MESH)
    for d in range(1, mates):
        pl.semaphore_signal(barrier, inc=1, device_id=mate_id(mate(d)), device_id_type=MESH)

    cuts = (0, 1 + groups // 2, 1 + groups)

    def received(sem, *region):
        whole = codes.at[region]
        pltpu.make_async_remote_copy(
            src_ref=whole, dst_ref=whole, send_sem=cs.at[0], recv_sem=sem,
            device_id=row_id(row_peer(1)), device_id_type=MESH).wait_recv()

    def sent(sem, ref):
        pltpu.make_async_remote_copy(
            src_ref=ref, dst_ref=ref, send_sem=sem, recv_sem=rr.at[0],
            device_id=row_id(row_peer(1)), device_id_type=MESH).wait_send()

    def half_unit(w, h):
        tiles = codes.at[r * windows + w, pl.ds(cuts[h], cuts[h + 1] - cuts[h])]
        return pltpu.make_async_remote_copy(
            src_ref=tiles, dst_ref=tiles, send_sem=cs.at[0], recv_sem=pr.at[h],
            device_id=row_id(w), device_id_type=MESH)

    def unit(s, w, q, relay):
        return pltpu.make_async_remote_copy(
            src_ref=codes.at[s * windows + w], dst_ref=codes.at[s * windows + w],
            send_sem=rest.at[0], recv_sem=rr.at[0] if relay else cr.at[w],
            device_id=row_id(q), device_id_type=MESH)

    def gain(s, q):
        return pltpu.make_async_remote_copy(
            src_ref=gains.at[s], dst_ref=gains.at[s], send_sem=gs.at[0],
            recv_sem=gr.at[0], device_id=row_id(q), device_id_type=MESH)

    row = lax.broadcasted_iota(jnp.int32, (groups, LANES), 0)
    own_day = r * days + lax.broadcasted_iota(jnp.int32, (days, LANES), 0)

    def encode(w):
        def load(g):
            x = held[w, :, lanes(g)]
            return jnp.where(own_day >= begins[w, :, lanes(g)], x, x[days - 1:days])

        centers = jnp.zeros((groups, LANES), jnp.float32)
        reach = jnp.full((1, LANES), TINY, jnp.float32)
        middles = []
        for g in range(groups):
            x = load(g)
            top = jnp.max(x, axis=0, keepdims=True)
            low = jnp.min(x, axis=0, keepdims=True)
            center = jnp.round((top + low) * (0.5 * TOP / LIMIT))
            middle = center * (LIMIT / TOP)
            reach = jnp.maximum(reach, jnp.maximum(top - middle, middle - low))
            centers = jnp.where(row == g, center, centers)
            middles.append(middle)
        codes[r * windows + w, 0] = centers.astype(jnp.int32).astype(jnp.int16)
        gains[r, w] = reach * (1.0 / TOP)
        inverse = TOP / reach
        for g in range(groups):
            codes[r * windows + w, 1 + g] = jnp.round((load(g) - middles[g]) * inverse).astype(jnp.int32).astype(jnp.int16)

    plans = [background(rows, windows, x) for x in range(rows)]

    def per_row(act):
        for x in range(rows):
            @pl.when(r == x)
            def _():
                act(x)

    def stage(number):
        def act(x):
            for s, w, q, when in plans[x]:
                if when == number:
                    if s != x and w != x:
                        received(rr.at[0], s * windows + w)
                    unit(s, w, q, s == x == w and abs(q - x) == rows - 1).start()

        per_row(act)

    pltpu.make_async_copy(begins, begins, bs.at[0]).wait()
    for i, w in enumerate(order):
        loads[i].wait()
        encode(w)
        if i == 1:
            pl.semaphore_wait(barrier, rows - 1 + mates - 1)
        if i > 0:
            half_unit(order[i - 1], 0).start()
    for w in order[:-1]:
        half_unit(w, 1).start()
    for d in range(1, rows):
        gain(r, row_peer(d)).start()
    stage(0)

    load_firsts.wait()
    lhs[:k] = firsts[...].astype(jnp.bfloat16)
    sent(cs.at[0], codes.at[pl.ds(0, rows - 1)])
    for d in range(1, subs):
        pl.semaphore_signal(clear, inc=1, device_id={"sub": lax.rem(lax.axis_index("sub") + d, subs)},
                            device_id_type=MESH)
    pl.semaphore_wait(clear, subs - 1)
    stage(1)

    day = lax.broadcasted_iota(jnp.int32, (total, LANES), 0)

    def standardize(w, store, some=range(groups)):
        middles = [codes[s * windows + w, 0].astype(jnp.float32) * (LIMIT / TOP) for s in range(rows)]
        steps = [gains[s, w] for s in range(rows)]
        for g in some:
            x = jnp.concatenate([
                codes[s * windows + w, 1 + g].astype(jnp.float32) * steps[s] + middles[s][g:g + 1]
                for s in range(rows)], axis=0)
            begin = begins[w, :, lanes(g)]
            live = day >= begin
            counts = (total - begin).astype(jnp.float32)
            mean = jnp.sum(jnp.where(live, x, 0.0), axis=0, keepdims=True) / counts
            centered = jnp.where(live, x - mean, 0.0)
            squares = jnp.sum(centered * centered, axis=0, keepdims=True)
            store(g, (centered * lax.rsqrt(squares + 1.0)).astype(jnp.bfloat16))

    def keep_own(g, value):
        lhs[k:, lanes(g)] = value

    some_gains = gains.at[pl.ds(0, rows - 1)]
    pltpu.make_async_remote_copy(
        src_ref=some_gains, dst_ref=some_gains, send_sem=gs.at[0], recv_sem=gr.at[0],
        device_id=row_id(row_peer(1)), device_id_type=MESH).wait_recv()
    sums = jnp.zeros((k + total, total), jnp.float32)
    for h in range(2):
        received(pr.at[h], pl.ds(0, rows - 1), pl.ds(cuts[h], cuts[h + 1] - cuts[h]))
        standardize(r, keep_own, range(h * groups // 2, (h + 1) * groups // 2))
        side = slice(h * width // 2, (h + 1) * width // 2)
        sums = sums + lax.dot_general(lhs[:, side], lhs[k:, side], NT, preferred_element_type=jnp.float32)
    summed = jnp.concatenate([sums[:half], sums[half:]], axis=1)
    mine[...] = summed
    for d in range(1, mates):
        pltpu.make_async_remote_copy(
            src_ref=mine, dst_ref=quad.at[m], send_sem=qs.at[0], recv_sem=qr.at[0],
            device_id=mate_id(mate(d)), device_id_type=MESH).start()
    quad[m] = summed
    stage(2)
    others = pltpu.make_async_remote_copy(
        src_ref=quad.at[pl.ds(0, mates - 1)], dst_ref=quad.at[pl.ds(0, mates - 1)],
        send_sem=qs.at[0], recv_sem=qr.at[0], device_id=mate_id(mate(1)), device_id_type=MESH)
    others.wait_recv()
    both = quad[0]
    for q in range(1, mates):
        both = both + quad[q]
    both = jnp.concatenate([both[:, :total], both[:, total:]], axis=0)
    proj, corr = both[:k], both[k:]
    image = exact(proj, corr)
    for step in range(ITERS):
        gram = lax.dot_general(image, proj, NT, precision=HIGHEST,
                               preferred_element_type=jnp.float32) / assets
        if step < ITERS - 1:
            proj, image = eliminate(gram, [image, exact(image, corr)])
        else:
            proj, = eliminate(gram, [proj])
    high = proj.astype(jnp.bfloat16)
    low = (proj - high.astype(jnp.float32)).astype(jnp.bfloat16)
    mix[r] = jnp.concatenate([high, low], axis=0)

    def deliver(slot, q):
        return pltpu.make_async_remote_copy(
            src_ref=mix.at[slot], dst_ref=mix.at[slot], send_sem=ms.at[0], recv_sem=mr.at[slot],
            device_id=row_id(q), device_id_type=MESH)

    def spread(x):
        for q in range(rows):
            if x in wanted(windows, q):
                deliver(x, q).start()

    per_row(spread)
    stage(3)

    def loadings(w, scaled):
        wide = jnp.dot(mix[w], scaled, preferred_element_type=jnp.float32)
        return (wide[:k] + wide[k:]).astype(jnp.bfloat16)

    part = width // PIECES

    def hand(h, side):
        return pltpu.make_async_remote_copy(
            src_ref=made.at[h], dst_ref=got.at[side, h], send_sem=hs.at[0], recv_sem=hr.at[side, h],
            device_id=row_id(r + 1 - 2 * side), device_id_type=MESH)

    def inner(row):
        return jnp.logical_and(row > 0, row < rows - 1)

    for h in range(PIECES):
        some = slice(h * part, (h + 1) * part)
        value = loadings(r, lhs[k:, some])
        made[h] = value

        @pl.when(inner(r))
        def _():
            for side in (0, 1):
                hand(h, side).start()

        out_ref[r, :, some] = value.astype(jnp.float32)

    lists = [wanted(windows, x) for x in range(rows)]
    most = max(len(v) for v in lists)
    for act in ("scale", "expand"):
        for j in range(most):
            have = [x for x in range(rows) if len(lists[x]) > j]
            w = sum(jnp.where(r == x, lists[x][j], 0) for x in have)

            @pl.when(functools.reduce(jnp.logical_or, [r == x for x in have]))
            def _():
                if act == "expand":
                    deliver(w, w).wait_recv()
                    out_ref[w] = loadings(w, sbuf[j]).astype(jnp.float32)
                    return

                part_only = [x for x in have if any(p[0] != x and p[1] == lists[x][j] for p in plans[x] if p[3] == 3)]
                fewer = functools.reduce(jnp.logical_or, [r == x for x in part_only], False)
                for count, flag in ((rows - 2, fewer), (rows - 1, jnp.logical_not(fewer))):
                    @pl.when(flag)
                    def _():
                        received(cr.at[w], pl.ds(0, count))

                def keep(g, value):
                    sbuf[j, :, lanes(g)] = value

                standardize(w, keep)

    def collect(side):
        for h in range(PIECES):
            hand(h, side).wait_recv()
            out_ref[r - 1 + 2 * side, :, h * part:(h + 1) * part] = got[side, h].astype(jnp.float32)

    for side in (0, 1):
        @pl.when(inner(r - 1 + 2 * side))
        def _():
            collect(side)

    others.wait_send()
    sent(gs.at[0], gains.at[pl.ds(0, rows - 1)])

    def settle(x):
        count = sum(x in wanted(windows, q) for q in range(rows))
        sent(ms.at[0], mix.at[pl.ds(0, count)])
        sent(rest.at[0], codes.at[pl.ds(0, len(plans[x]))])

    per_row(settle)

    @pl.when(inner(r))
    def _():
        sent(hs.at[0], got)


def fused(returns, starts, start_block, rows, cols, subs):
    windows, days, width = returns.shape
    k = start_block.shape[1]
    total = days * rows
    mates = cols * subs
    half = (k + total) // 2
    groups = width // LANES
    f32, bf16 = jnp.float32, jnp.bfloat16
    dma = pltpu.SemaphoreType.DMA
    return pl.pallas_call(
        functools.partial(kernel, rows, cols, subs, width * mates),
        out_shape=pltpu.VMEM(start_block.shape, f32),
        in_specs=[pl.BlockSpec(memory_space=pl.ANY)] * 3,
        out_specs=pl.BlockSpec(memory_space=pltpu.VMEM),
        scratch_shapes=[
            pltpu.VMEM(returns.shape, f32),
            pltpu.VMEM((windows, 1, width), jnp.int32),
            pltpu.VMEM((k, width), f32),
            pltpu.VMEM((rows * windows, groups + 1, days, LANES), jnp.int16),
            pltpu.VMEM((k + total, width), bf16),
            pltpu.VMEM((windows - 2, total, width), bf16),
            pltpu.VMEM((half, 2 * total), f32),
            pltpu.VMEM((mates, half, 2 * total), f32),
            pltpu.VMEM((windows, 2 * k, total), bf16),
            pltpu.VMEM((rows, windows, 1, LANES), f32),
            pltpu.VMEM((PIECES, k, width // PIECES), bf16),
            pltpu.VMEM((2, PIECES, k, width // PIECES), bf16),
            dma((windows,)), dma((2,)),
            dma((1,)), dma((2,)), dma((windows,)), dma((1,)),
            dma((1,)), dma((1,)), dma((1,)), dma((windows,)),
            dma((1,)), dma((1,)), dma((1,)), dma((1,)), dma((2, PIECES)),
            pltpu.SemaphoreType.REGULAR,
        ],
        compiler_params=pltpu.CompilerParams(collective_id=0, has_side_effects=True),
    )(returns, starts, start_block)


def gram_of(image):
    return jnp.einsum("wkj,wlj->wkl", image, image, precision=HIGHEST)


def project(factors, scaled):
    rounded = factors.astype(jnp.bfloat16)
    return jnp.einsum("wka,wta->wkt", rounded, scaled, preferred_element_type=jnp.float32)


def expand(proj, widened):
    return jnp.einsum("wkt,wta->wka", proj, widened, precision=HIGHEST)


def orthonormal(image, gram, assets):
    lower = jnp.linalg.cholesky(gram / assets)
    return jax.scipy.linalg.solve_triangular(lower, image, lower=True)


def stepwise(returns, starts, start_block, rows, mates):
    windows, days, width = returns.shape
    row_pos = lax.axis_index("rows")
    total_days = days * rows
    day_index = row_pos * days + jnp.arange(days, dtype=jnp.int32)
    live = (day_index[None, :, None] >= starts[:, None, :]).astype(jnp.float32)
    counts = (total_days - starts).astype(jnp.float32)
    masked = live * returns
    sums = lax.psum(jnp.sum(masked, axis=1), "rows")
    mean = sums / counts
    centered = live * (returns - mean[:, None, :])
    squares = lax.psum(jnp.sum(centered * centered, axis=1), "rows")
    scaled = (centered * lax.rsqrt(squares + 1.0)[:, None, :]).astype(jnp.bfloat16)
    widened = scaled.astype(jnp.float32)
    factors = start_block
    for step in range(ITERS):
        proj = lax.psum(project(factors, scaled), ("cols", "sub"))
        image = lax.psum(expand(proj, widened), "rows")
        gram = lax.psum(gram_of(image), ("cols", "sub"))
        factors = orthonormal(image, gram, width * mates)
    return factors


def on_device(rows, cols, subs, returns, starts, start_block):
    windows, days, width = returns.shape
    k = start_block.shape[1]
    fits = (windows == rows and width == LANES * days and days % 16 == 0 and k % 16 == 0
            and days * rows <= 64 and (days * rows + k) % 16 == 0 and rows == 4 and cols * subs > 1)
    if fits:
        return fused(returns, starts, start_block, rows, cols, subs)
    return stepwise(returns, starts, start_block, rows, cols * subs)


def solution(mesh):
    placed = (
        P("groups", "rows", ("cols", "sub")),
        P("groups", ("cols", "sub")),
        P("groups", None, ("cols", "sub")),
    )
    sizes = (mesh.shape["rows"], mesh.shape["cols"], mesh.shape["sub"])
    return jax.shard_map(
        functools.partial(on_device, *sizes),
        mesh=mesh,
        in_specs=placed,
        out_specs=P("groups", None, ("cols", "sub")),
        check_vma=False,
    )
```

```python
import functools

import jax
import jax.numpy as jnp
from jax import lax
from jax.experimental import pallas as pl
from jax.experimental.pallas import tpu as pltpu
from jax.sharding import PartitionSpec as P

ITERS = 3
HIGHEST = lax.Precision.HIGHEST
MESH = pl.DeviceIdType.MESH
NT = (((1,), (1,)), ((), ()))
SUBLANES = 8
LANES = 128
LIMIT = 6.0
TOP = 32767.0
TINY = 1e-30
PIECES = 2


def eliminate(gram, rights):
    size, wide = gram.shape[0], rights[0].shape[1]
    tiles = size // SUBLANES
    sums = [[x[c * SUBLANES:(c + 1) * SUBLANES] for c in range(tiles)] for x in rights]
    row_id = lax.broadcasted_iota(jnp.int32, (SUBLANES, 1), 0)
    diag = [jnp.ones((SUBLANES, wide), jnp.float32) for _ in range(tiles)]
    panel = {
        (c, i): jnp.broadcast_to(gram[c * SUBLANES:(c + 1) * SUBLANES, i:i + 1], (SUBLANES, wide))
        for i in range(size) for c in range(i // SUBLANES, tiles)
    }
    for i in range(size):
        own, sub = i // SUBLANES, i % SUBLANES
        pivot = panel[own, i][sub:sub + 1]
        inverse = 1.0 / pivot
        diag[own] = jnp.where(row_id == sub, pivot, diag[own])
        ahead = {n: panel[n // SUBLANES, i][n % SUBLANES:n % SUBLANES + 1] for n in range(i + 1, size)}
        rows = [x[own][sub:sub + 1] for x in sums]
        for c in range(own, tiles):
            factor = panel[c, i] * inverse
            if c == own:
                factor = jnp.where(row_id > sub, factor, 0.0)
            for n in range(i + 1, size):
                if c >= n // SUBLANES:
                    panel[c, n] = panel[c, n] - factor * ahead[n]
            for x, row in zip(sums, rows):
                x[c] = x[c] - factor * row
    roots = [lax.rsqrt(d) for d in diag]
    return [jnp.concatenate([v * d for v, d in zip(x, roots)], axis=0) for x in sums]


def exact(left, right):
    return jnp.dot(left, right, precision=HIGHEST, preferred_element_type=jnp.float32)


def wanted(windows, x):
    some = [w for w in range(windows) if w != x and (abs(w - x) > 1 or w in (0, windows - 1))]
    return some if x >= windows // 2 else some[::-1]


def background(rows, windows, x):
    ends = (0, rows - 1)
    plan = []
    for q in range(rows):
        for w in wanted(windows, q) if q != x else []:
            if q in ends:
                plan.append((x, w, q, 0 if abs(q - x) == 1 else 1))
            elif x in ends and abs(q - x) == 1:
                plan.append((x, w, q, 2 if w == x else 0))
            elif abs(q - x) == 1 and abs(w - q) > 1:
                plan.append((x, w, q, 1))
    if x in ends:
        near = 1 if x == 0 else rows - 2
        for s in range(rows):
            if s not in (x, near):
                plan.append((s, x, near, 2))
                plan += [(s, w, near, 3) for w in wanted(windows, near) if w == s]
    return plan


def kernel(rows, cols, subs, assets,
           returns_ref, starts_ref, start_ref, out_ref,
           held, begins, firsts, codes, lhs, sbuf, mine, quad, mix, gains, made, got,
           ls, bs, cs, pr, cr, rr, qs, qr, ms, mr, gs, gr, rest, hs, hr, clear, ready):
    r = lax.axis_index("rows")
    mates = cols * subs
    m = lax.axis_index("cols") * subs + lax.axis_index("sub")
    windows, days, width = returns_ref.shape
    k = start_ref.shape[1]
    total = days * rows
    groups = width // LANES
    half = (k + total) // 2
    def row_peer(d):
        return lax.rem(r + d, rows)

    def mate(d):
        return lax.rem(m + d, mates)

    def row_id(q):
        return {"rows": q}

    def mate_id(q):
        return {"cols": q // subs, "sub": lax.rem(q, subs)}

    def lanes(g):
        return slice(g * LANES, (g + 1) * LANES)

    order = [row_peer(d) for d in sorted(range(rows), key=lambda d: -min(d, rows - d))]
    load_begins = [pltpu.make_async_copy(starts_ref.at[pl.ds(w, 1)], begins.at[w], bs.at[0]) for w in range(windows)]
    for c in load_begins:
        c.start()
    loads = [pltpu.make_async_copy(returns_ref.at[w], held.at[w], ls.at[w]) for w in order]
    for c in loads:
        c.start()
    load_firsts = pltpu.make_async_copy(start_ref.at[r], firsts, bs.at[1])
    load_firsts.start()

    barrier = pltpu.get_barrier_semaphore()
    for step in (1, -1):
        @pl.when(r + step < rows if step > 0 else r > 0)
        def _():
            pl.semaphore_signal(barrier, inc=1, device_id=row_id(r + step), device_id_type=MESH)

    for d in range(1, mates):
        pl.semaphore_signal(barrier, inc=1, device_id=mate_id(mate(d)), device_id_type=MESH)

    cuts = (0, 1 + groups // 2, 1 + groups)

    def received(sem, *region):
        whole = codes.at[region]
        pltpu.make_async_remote_copy(
            src_ref=whole, dst_ref=whole, send_sem=cs.at[0], recv_sem=sem,
            device_id=row_id(row_peer(1)), device_id_type=MESH).wait_recv()

    def sent(sem, ref):
        pltpu.make_async_remote_copy(
            src_ref=ref, dst_ref=ref, send_sem=sem, recv_sem=rr.at[0],
            device_id=row_id(row_peer(1)), device_id_type=MESH).wait_send()

    def half_unit(w, h):
        tiles = codes.at[r * windows + w, pl.ds(cuts[h], cuts[h + 1] - cuts[h])]
        return pltpu.make_async_remote_copy(
            src_ref=tiles, dst_ref=tiles, send_sem=cs.at[0], recv_sem=pr.at[h],
            device_id=row_id(w), device_id_type=MESH)

    def unit(s, w, q, relay):
        return pltpu.make_async_remote_copy(
            src_ref=codes.at[s * windows + w], dst_ref=codes.at[s * windows + w],
            send_sem=rest.at[0], recv_sem=rr.at[0] if relay else cr.at[w],
            device_id=row_id(q), device_id_type=MESH)

    def gain(s, q):
        return pltpu.make_async_remote_copy(
            src_ref=gains.at[s], dst_ref=gains.at[s], send_sem=gs.at[0],
            recv_sem=gr.at[0], device_id=row_id(q), device_id_type=MESH)

    row = lax.broadcasted_iota(jnp.int32, (groups, LANES), 0)
    own_day = r * days + lax.broadcasted_iota(jnp.int32, (days, LANES), 0)

    def encode(w):
        def load(g):
            x = held[w, :, lanes(g)]
            return jnp.where(own_day >= begins[w, :, lanes(g)], x, x[days - 1:days])

        centers = jnp.zeros((groups, LANES), jnp.float32)
        reach = jnp.full((1, LANES), TINY, jnp.float32)
        middles = []
        for g in range(groups):
            x = load(g)
            top = jnp.max(x, axis=0, keepdims=True)
            low = jnp.min(x, axis=0, keepdims=True)
            center = jnp.round((top + low) * (0.5 * TOP / LIMIT))
            middle = center * (LIMIT / TOP)
            reach = jnp.maximum(reach, jnp.maximum(top - middle, middle - low))
            centers = jnp.where(row == g, center, centers)
            middles.append(middle)
        codes[r * windows + w, 0] = centers.astype(jnp.int32).astype(jnp.int16)
        gains[r, w] = reach * (1.0 / TOP)
        inverse = TOP / reach
        for g in range(groups):
            codes[r * windows + w, 1 + g] = jnp.round((load(g) - middles[g]) * inverse).astype(jnp.int32).astype(jnp.int16)

    plans = [background(rows, windows, x) for x in range(rows)]

    def per_row(act):
        for x in range(rows):
            @pl.when(r == x)
            def _():
                act(x)

    def stage(number, some=range(rows)):
        def act(x):
            for s, w, q, when in plans[x]:
                if when == number and x in some:
                    if s != x and w != x:
                        received(rr.at[0], s * windows + w)
                    unit(s, w, q, s == x == w and abs(q - x) == rows - 1).start()

        per_row(act)

    pltpu.make_async_copy(begins, begins, bs.at[0]).wait()
    for i, w in enumerate(order):
        loads[i].wait()
        encode(w)
    pl.semaphore_wait(barrier, mates - 1 + jnp.where(jnp.logical_or(r == 0, r == rows - 1), 1, 2))

    def reach_out(x):
        for t in range(1, rows):
            for step in (1, -1):
                if 0 <= x - step * t < rows and 0 <= x + step < rows and t + 1 < rows:
                    pl.semaphore_signal(ready.at[0 if step > 0 else 1, t + 1], inc=1,
                                        device_id=row_id(x + step), device_id_type=MESH)
            for q in (x + t, x - t):
                if 0 <= q < rows:
                    half_unit(q, 0).start()
                    half_unit(q, 1).start()
                    gain(r, q).start()
            if t == (rows - 1 if x in (0, rows - 1) else 1):
                for s, w, q, when in plans[x]:
                    if when == 0:
                        unit(s, w, q, False).start()
            for side, far in ((0, x - t - 1), (1, x + t + 1)):
                if 0 <= far < rows:
                    pl.semaphore_wait(ready.at[side, t + 1], 1)

    per_row(reach_out)

    load_firsts.wait()
    lhs[:k] = firsts[...].astype(jnp.bfloat16)
    sent(cs.at[0], codes.at[pl.ds(0, rows - 1)])
    for d in range(1, subs):
        pl.semaphore_signal(clear, inc=1, device_id={"sub": lax.rem(lax.axis_index("sub") + d, subs)},
                            device_id_type=MESH)
    pl.semaphore_wait(clear, subs - 1)
    held_back = (0, rows - 2)
    stage(1, [x for x in range(rows) if x not in held_back])

    day = lax.broadcasted_iota(jnp.int32, (total, LANES), 0)

    def standardize(w, store, some=range(groups)):
        middles = [codes[s * windows + w, 0].astype(jnp.float32) * (LIMIT / TOP) for s in range(rows)]
        steps = [gains[s, w] for s in range(rows)]
        for g in some:
            x = jnp.concatenate([
                codes[s * windows + w, 1 + g].astype(jnp.float32) * steps[s] + middles[s][g:g + 1]
                for s in range(rows)], axis=0)
            begin = begins[w, :, lanes(g)]
            live = day >= begin
            counts = (total - begin).astype(jnp.float32)
            mean = jnp.sum(jnp.where(live, x, 0.0), axis=0, keepdims=True) / counts
            centered = jnp.where(live, x - mean, 0.0)
            squares = jnp.sum(centered * centered, axis=0, keepdims=True)
            store(g, (centered * lax.rsqrt(squares + 1.0)).astype(jnp.bfloat16))

    def keep_own(g, value):
        lhs[k:, lanes(g)] = value

    some_gains = gains.at[pl.ds(0, rows - 1)]
    pltpu.make_async_remote_copy(
        src_ref=some_gains, dst_ref=some_gains, send_sem=gs.at[0], recv_sem=gr.at[0],
        device_id=row_id(row_peer(1)), device_id_type=MESH).wait_recv()
    sums = jnp.zeros((k + total, total), jnp.float32)
    for h in range(2):
        received(pr.at[h], pl.ds(0, rows - 1), pl.ds(cuts[h], cuts[h + 1] - cuts[h]))
        if h == 1:
            stage(1, held_back)
        standardize(r, keep_own, range(h * groups // 2, (h + 1) * groups // 2))
        side = slice(h * width // 2, (h + 1) * width // 2)
        sums = sums + lax.dot_general(lhs[:, side], lhs[k:, side], NT, preferred_element_type=jnp.float32)
    summed = jnp.concatenate([sums[:half], sums[half:]], axis=1)
    mine[...] = summed
    for d in range(1, mates):
        pltpu.make_async_remote_copy(
            src_ref=mine, dst_ref=quad.at[m], send_sem=qs.at[0], recv_sem=qr.at[0],
            device_id=mate_id(mate(d)), device_id_type=MESH).start()
    quad[m] = summed
    stage(2)
    others = pltpu.make_async_remote_copy(
        src_ref=quad.at[pl.ds(0, mates - 1)], dst_ref=quad.at[pl.ds(0, mates - 1)],
        send_sem=qs.at[0], recv_sem=qr.at[0], device_id=mate_id(mate(1)), device_id_type=MESH)
    others.wait_recv()
    both = quad[0]
    for q in range(1, mates):
        both = both + quad[q]
    both = jnp.concatenate([both[:, :total], both[:, total:]], axis=0)
    proj, corr = both[:k], both[k:]
    image = exact(proj, corr)
    for step in range(ITERS):
        gram = lax.dot_general(image, proj, NT, precision=HIGHEST,
                               preferred_element_type=jnp.float32) / assets
        if step < ITERS - 1:
            proj, image = eliminate(gram, [image, exact(image, corr)])
        else:
            proj, = eliminate(gram, [proj])
    high = proj.astype(jnp.bfloat16)
    low = (proj - high.astype(jnp.float32)).astype(jnp.bfloat16)
    mix[r] = jnp.concatenate([high, low], axis=0)

    def deliver(slot, q):
        return pltpu.make_async_remote_copy(
            src_ref=mix.at[slot], dst_ref=mix.at[slot], send_sem=ms.at[0], recv_sem=mr.at[slot],
            device_id=row_id(q), device_id_type=MESH)

    def spread(x):
        for q in range(rows):
            if x in wanted(windows, q):
                deliver(x, q).start()

    per_row(spread)
    stage(3)

    def loadings(w, scaled):
        wide = jnp.dot(mix[w], scaled, preferred_element_type=jnp.float32)
        return (wide[:k] + wide[k:]).astype(jnp.bfloat16)

    part = width // PIECES

    def hand(h, side):
        return pltpu.make_async_remote_copy(
            src_ref=made.at[h], dst_ref=got.at[side, h], send_sem=hs.at[0], recv_sem=hr.at[side, h],
            device_id=row_id(r + 1 - 2 * side), device_id_type=MESH)

    def inner(row):
        return jnp.logical_and(row > 0, row < rows - 1)

    for h in range(PIECES):
        some = slice(h * part, (h + 1) * part)
        value = loadings(r, lhs[k:, some])
        made[h] = value

        @pl.when(inner(r))
        def _():
            for side in (0, 1):
                hand(h, side).start()

        out_ref[r, :, some] = value.astype(jnp.float32)

    lists = [wanted(windows, x) for x in range(rows)]
    most = max(len(v) for v in lists)
    for act in ("scale", "expand"):
        for j in range(most):
            have = [x for x in range(rows) if len(lists[x]) > j]
            w = sum(jnp.where(r == x, lists[x][j], 0) for x in have)

            @pl.when(functools.reduce(jnp.logical_or, [r == x for x in have]))
            def _():
                if act == "expand":
                    deliver(w, w).wait_recv()
                    out_ref[w] = loadings(w, sbuf[j]).astype(jnp.float32)
                    return

                part_only = [x for x in have if any(p[0] != x and p[1] == lists[x][j] for p in plans[x] if p[3] == 3)]
                fewer = functools.reduce(jnp.logical_or, [r == x for x in part_only], False)
                for count, flag in ((rows - 2, fewer), (rows - 1, jnp.logical_not(fewer))):
                    @pl.when(flag)
                    def _():
                        received(cr.at[w], pl.ds(0, count))

                def keep(g, value):
                    sbuf[j, :, lanes(g)] = value

                standardize(w, keep)

    def collect(side):
        for h in range(PIECES):
            hand(h, side).wait_recv()
            out_ref[r - 1 + 2 * side, :, h * part:(h + 1) * part] = got[side, h].astype(jnp.float32)

    for side in (0, 1):
        @pl.when(inner(r - 1 + 2 * side))
        def _():
            collect(side)

    others.wait_send()
    sent(gs.at[0], gains.at[pl.ds(0, rows - 1)])

    def settle(x):
        count = sum(x in wanted(windows, q) for q in range(rows))
        sent(ms.at[0], mix.at[pl.ds(0, count)])
        sent(rest.at[0], codes.at[pl.ds(0, len(plans[x]))])

    per_row(settle)

    @pl.when(inner(r))
    def _():
        sent(hs.at[0], got)


def fused(returns, starts, start_block, rows, cols, subs):
    windows, days, width = returns.shape
    k = start_block.shape[1]
    total = days * rows
    mates = cols * subs
    half = (k + total) // 2
    groups = width // LANES
    f32, bf16 = jnp.float32, jnp.bfloat16
    dma = pltpu.SemaphoreType.DMA
    return pl.pallas_call(
        functools.partial(kernel, rows, cols, subs, width * mates),
        out_shape=pltpu.VMEM(start_block.shape, f32),
        in_specs=[pl.BlockSpec(memory_space=pl.ANY)] * 3,
        out_specs=pl.BlockSpec(memory_space=pltpu.VMEM),
        scratch_shapes=[
            pltpu.VMEM(returns.shape, f32),
            pltpu.VMEM((windows, 1, width), jnp.int32),
            pltpu.VMEM((k, width), f32),
            pltpu.VMEM((rows * windows, groups + 1, days, LANES), jnp.int16),
            pltpu.VMEM((k + total, width), bf16),
            pltpu.VMEM((windows - 2, total, width), bf16),
            pltpu.VMEM((half, 2 * total), f32),
            pltpu.VMEM((mates, half, 2 * total), f32),
            pltpu.VMEM((windows, 2 * k, total), bf16),
            pltpu.VMEM((rows, windows, 1, LANES), f32),
            pltpu.VMEM((PIECES, k, width // PIECES), bf16),
            pltpu.VMEM((2, PIECES, k, width // PIECES), bf16),
            dma((windows,)), dma((2,)),
            dma((1,)), dma((2,)), dma((windows,)), dma((1,)),
            dma((1,)), dma((1,)), dma((1,)), dma((windows,)),
            dma((1,)), dma((1,)), dma((1,)), dma((1,)), dma((2, PIECES)),
            pltpu.SemaphoreType.REGULAR, pltpu.SemaphoreType.REGULAR((2, rows)),
        ],
        compiler_params=pltpu.CompilerParams(collective_id=0, has_side_effects=True),
    )(returns, starts, start_block)


def gram_of(image):
    return jnp.einsum("wkj,wlj->wkl", image, image, precision=HIGHEST)


def project(factors, scaled):
    rounded = factors.astype(jnp.bfloat16)
    return jnp.einsum("wka,wta->wkt", rounded, scaled, preferred_element_type=jnp.float32)


def expand(proj, widened):
    return jnp.einsum("wkt,wta->wka", proj, widened, precision=HIGHEST)


def orthonormal(image, gram, assets):
    lower = jnp.linalg.cholesky(gram / assets)
    return jax.scipy.linalg.solve_triangular(lower, image, lower=True)


def stepwise(returns, starts, start_block, rows, mates):
    windows, days, width = returns.shape
    row_pos = lax.axis_index("rows")
    total_days = days * rows
    day_index = row_pos * days + jnp.arange(days, dtype=jnp.int32)
    live = (day_index[None, :, None] >= starts[:, None, :]).astype(jnp.float32)
    counts = (total_days - starts).astype(jnp.float32)
    masked = live * returns
    sums = lax.psum(jnp.sum(masked, axis=1), "rows")
    mean = sums / counts
    centered = live * (returns - mean[:, None, :])
    squares = lax.psum(jnp.sum(centered * centered, axis=1), "rows")
    scaled = (centered * lax.rsqrt(squares + 1.0)[:, None, :]).astype(jnp.bfloat16)
    widened = scaled.astype(jnp.float32)
    factors = start_block
    for step in range(ITERS):
        proj = lax.psum(project(factors, scaled), ("cols", "sub"))
        image = lax.psum(expand(proj, widened), "rows")
        gram = lax.psum(gram_of(image), ("cols", "sub"))
        factors = orthonormal(image, gram, width * mates)
    return factors


def on_device(rows, cols, subs, returns, starts, start_block):
    windows, days, width = returns.shape
    k = start_block.shape[1]
    fits = (windows == rows and width == LANES * days and days % 16 == 0 and k % 16 == 0
            and days * rows <= 64 and (days * rows + k) % 16 == 0 and rows == 4 and cols * subs > 1)
    if fits:
        return fused(returns, starts, start_block, rows, cols, subs)
    return stepwise(returns, starts, start_block, rows, cols * subs)


def solution(mesh):
    placed = (
        P("groups", "rows", ("cols", "sub")),
        P("groups", ("cols", "sub")),
        P("groups", None, ("cols", "sub")),
    )
    sizes = (mesh.shape["rows"], mesh.shape["cols"], mesh.shape["sub"])
    return jax.shard_map(
        functools.partial(on_device, *sizes),
        mesh=mesh,
        in_specs=placed,
        out_specs=P("groups", None, ("cols", "sub")),
        check_vma=False,
    )
```

```python
import functools

import jax
import jax.numpy as jnp
from jax import lax
from jax.experimental import pallas as pl
from jax.experimental.pallas import tpu as pltpu
from jax.sharding import PartitionSpec as P

ITERS = 3
HIGHEST = lax.Precision.HIGHEST
MESH = pl.DeviceIdType.MESH
NT = (((1,), (1,)), ((), ()))
SUBLANES = 8
LANES = 128
LIMIT = 6.0
TOP = 32767.0
TINY = 1e-30
PIECES = 2


def eliminate(gram, rights):
    size, wide = gram.shape[0], rights[0].shape[1]
    tiles = size // SUBLANES
    sums = [[x[c * SUBLANES:(c + 1) * SUBLANES] for c in range(tiles)] for x in rights]
    row_id = lax.broadcasted_iota(jnp.int32, (SUBLANES, 1), 0)
    diag = [jnp.ones((SUBLANES, wide), jnp.float32) for _ in range(tiles)]
    panel = {
        (c, i): jnp.broadcast_to(gram[c * SUBLANES:(c + 1) * SUBLANES, i:i + 1], (SUBLANES, wide))
        for i in range(size) for c in range(i // SUBLANES, tiles)
    }
    for i in range(size):
        own, sub = i // SUBLANES, i % SUBLANES
        pivot = panel[own, i][sub:sub + 1]
        inverse = 1.0 / pivot
        diag[own] = jnp.where(row_id == sub, pivot, diag[own])
        ahead = {n: panel[n // SUBLANES, i][n % SUBLANES:n % SUBLANES + 1] for n in range(i + 1, size)}
        rows = [x[own][sub:sub + 1] for x in sums]
        for c in range(own, tiles):
            factor = panel[c, i] * inverse
            if c == own:
                factor = jnp.where(row_id > sub, factor, 0.0)
            for n in range(i + 1, size):
                if c >= n // SUBLANES:
                    panel[c, n] = panel[c, n] - factor * ahead[n]
            for x, row in zip(sums, rows):
                x[c] = x[c] - factor * row
    roots = [lax.rsqrt(d) for d in diag]
    return [jnp.concatenate([v * d for v, d in zip(x, roots)], axis=0) for x in sums]


def exact(left, right):
    return jnp.dot(left, right, precision=HIGHEST, preferred_element_type=jnp.float32)


def wanted(windows, x):
    some = [w for w in range(windows) if w != x and (abs(w - x) > 1 or w in (0, windows - 1))]
    return some if x >= windows // 2 else some[::-1]


def background(rows, windows, x):
    ends = (0, rows - 1)
    plan = []
    for q in range(rows):
        for w in wanted(windows, q) if q != x else []:
            if q in ends:
                plan.append((x, w, q, 0 if abs(q - x) == 1 else 1))
            elif x in ends and abs(q - x) == 1:
                plan.append((x, w, q, 2 if w == x else 0))
            elif abs(q - x) == 1 and abs(w - q) > 1:
                plan.append((x, w, q, 1))
    if x in ends:
        near = 1 if x == 0 else rows - 2
        for s in range(rows):
            if s not in (x, near):
                plan.append((s, x, near, 2))
                plan += [(s, w, near, 3) for w in wanted(windows, near) if w == s]
    return plan


def kernel(rows, cols, subs, assets,
           returns_ref, starts_ref, start_ref, out_ref,
           held, begins, firsts, codes, lhs, sbuf, mine, quad, mix, gains, made, got,
           ls, bs, cs, pr, cr, rr, qs, qr, ms, mr, gs, gr, rest, hs, hr, clear, ready):
    r = lax.axis_index("rows")
    mates = cols * subs
    m = lax.axis_index("cols") * subs + lax.axis_index("sub")
    windows, days, width = returns_ref.shape
    k = start_ref.shape[1]
    total = days * rows
    groups = width // LANES
    half = (k + total) // 2
    def row_peer(d):
        return lax.rem(r + d, rows)

    def mate(d):
        return lax.rem(m + d, mates)

    def row_id(q):
        return {"rows": q}

    def mate_id(q):
        return {"cols": q // subs, "sub": lax.rem(q, subs)}

    def lanes(g):
        return slice(g * LANES, (g + 1) * LANES)

    order = [row_peer(d) for d in sorted(range(rows), key=lambda d: -min(d, rows - d))]
    load_begins = [pltpu.make_async_copy(starts_ref.at[pl.ds(w, 1)], begins.at[w], bs.at[0]) for w in range(windows)]
    for c in load_begins:
        c.start()
    loads = [pltpu.make_async_copy(returns_ref.at[w], held.at[w], ls.at[w]) for w in order]
    for c in loads:
        c.start()
    load_firsts = pltpu.make_async_copy(start_ref.at[r], firsts, bs.at[1])
    load_firsts.start()

    barrier = pltpu.get_barrier_semaphore()
    for step in (1, -1):
        @pl.when(r + step < rows if step > 0 else r > 0)
        def _():
            pl.semaphore_signal(barrier, inc=1, device_id=row_id(r + step), device_id_type=MESH)

    for d in range(1, mates):
        pl.semaphore_signal(barrier, inc=1, device_id=mate_id(mate(d)), device_id_type=MESH)

    cuts = (0, 1 + groups // 2, 1 + groups)

    def received(sem, *region):
        whole = codes.at[region]
        pltpu.make_async_remote_copy(
            src_ref=whole, dst_ref=whole, send_sem=cs.at[0], recv_sem=sem,
            device_id=row_id(row_peer(1)), device_id_type=MESH).wait_recv()

    def sent(sem, ref):
        pltpu.make_async_remote_copy(
            src_ref=ref, dst_ref=ref, send_sem=sem, recv_sem=rr.at[0],
            device_id=row_id(row_peer(1)), device_id_type=MESH).wait_send()

    def half_unit(w, h):
        tiles = codes.at[r * windows + w, pl.ds(cuts[h], cuts[h + 1] - cuts[h])]
        return pltpu.make_async_remote_copy(
            src_ref=tiles, dst_ref=tiles, send_sem=cs.at[0], recv_sem=pr.at[h],
            device_id=row_id(w), device_id_type=MESH)

    def unit(s, w, q, relay):
        return pltpu.make_async_remote_copy(
            src_ref=codes.at[s * windows + w], dst_ref=codes.at[s * windows + w],
            send_sem=rest.at[0], recv_sem=rr.at[0] if relay else cr.at[w],
            device_id=row_id(q), device_id_type=MESH)

    def gain(s, q):
        return pltpu.make_async_remote_copy(
            src_ref=gains.at[s], dst_ref=gains.at[s], send_sem=gs.at[0],
            recv_sem=gr.at[0], device_id=row_id(q), device_id_type=MESH)

    row = lax.broadcasted_iota(jnp.int32, (groups, LANES), 0)
    own_day = r * days + lax.broadcasted_iota(jnp.int32, (days, LANES), 0)

    def encode(w):
        def load(g):
            x = held[w, :, lanes(g)]
            return jnp.where(own_day >= begins[w, :, lanes(g)], x, x[days - 1:days])

        centers = jnp.zeros((groups, LANES), jnp.float32)
        reach = jnp.full((1, LANES), TINY, jnp.float32)
        middles = []
        for g in range(groups):
            x = load(g)
            top = jnp.max(x, axis=0, keepdims=True)
            low = jnp.min(x, axis=0, keepdims=True)
            center = jnp.round((top + low) * (0.5 * TOP / LIMIT))
            middle = center * (LIMIT / TOP)
            reach = jnp.maximum(reach, jnp.maximum(top - middle, middle - low))
            centers = jnp.where(row == g, center, centers)
            middles.append(middle)
        codes[r * windows + w, 0] = centers.astype(jnp.int32).astype(jnp.int16)
        gains[r, w] = reach * (1.0 / TOP)
        inverse = TOP / reach
        for g in range(groups):
            codes[r * windows + w, 1 + g] = jnp.round((load(g) - middles[g]) * inverse).astype(jnp.int32).astype(jnp.int16)

    plans = [background(rows, windows, x) for x in range(rows)]

    def per_row(act):
        for x in range(rows):
            @pl.when(r == x)
            def _():
                act(x)

    def stage(number, some=range(rows)):
        def act(x):
            for s, w, q, when in plans[x]:
                if when == number and x in some:
                    if s != x and w != x:
                        received(rr.at[0], s * windows + w)
                    unit(s, w, q, s == x == w and abs(q - x) == rows - 1).start()

        per_row(act)

    pltpu.make_async_copy(begins, begins, bs.at[0]).wait()
    for i, w in enumerate(order):
        loads[i].wait()
        encode(w)
    pl.semaphore_wait(barrier, mates - 1 + jnp.where(jnp.logical_or(r == 0, r == rows - 1), 1, 2))

    def reach_out(x):
        for t in range(1, rows):
            for step in (1, -1):
                if 0 <= x - step * t < rows and 0 <= x + step < rows and t + 1 < rows:
                    pl.semaphore_signal(ready.at[0 if step > 0 else 1, t + 1], inc=1,
                                        device_id=row_id(x + step), device_id_type=MESH)
            for q in (x + t, x - t):
                if 0 <= q < rows:
                    half_unit(q, 0).start()
                    half_unit(q, 1).start()
                    gain(r, q).start()
            if t == (rows - 1 if x in (0, rows - 1) else 1):
                for s, w, q, when in plans[x]:
                    if when == 0:
                        unit(s, w, q, False).start()
            for side, far in ((0, x - t - 1), (1, x + t + 1)):
                if 0 <= far < rows:
                    pl.semaphore_wait(ready.at[side, t + 1], 1)

    per_row(reach_out)

    load_firsts.wait()
    lhs[:k] = firsts[...].astype(jnp.bfloat16)
    sent(cs.at[0], codes.at[pl.ds(0, rows - 1)])
    for d in range(1, subs):
        pl.semaphore_signal(clear, inc=1, device_id={"sub": lax.rem(lax.axis_index("sub") + d, subs)},
                            device_id_type=MESH)
    pl.semaphore_wait(clear, subs - 1)
    held_back = (0,)
    stage(1, [x for x in range(rows) if x not in held_back])

    day = lax.broadcasted_iota(jnp.int32, (total, LANES), 0)

    def standardize(w, store, some=range(groups)):
        middles = [codes[s * windows + w, 0].astype(jnp.float32) * (LIMIT / TOP) for s in range(rows)]
        steps = [gains[s, w] for s in range(rows)]
        for g in some:
            x = jnp.concatenate([
                codes[s * windows + w, 1 + g].astype(jnp.float32) * steps[s] + middles[s][g:g + 1]
                for s in range(rows)], axis=0)
            begin = begins[w, :, lanes(g)]
            live = day >= begin
            counts = (total - begin).astype(jnp.float32)
            mean = jnp.sum(jnp.where(live, x, 0.0), axis=0, keepdims=True) / counts
            centered = jnp.where(live, x - mean, 0.0)
            squares = jnp.sum(centered * centered, axis=0, keepdims=True)
            store(g, (centered * lax.rsqrt(squares + 1.0)).astype(jnp.bfloat16))

    def keep_own(g, value):
        lhs[k:, lanes(g)] = value

    some_gains = gains.at[pl.ds(0, rows - 1)]
    pltpu.make_async_remote_copy(
        src_ref=some_gains, dst_ref=some_gains, send_sem=gs.at[0], recv_sem=gr.at[0],
        device_id=row_id(row_peer(1)), device_id_type=MESH).wait_recv()
    sums = jnp.zeros((k + total, total), jnp.float32)
    for h in range(2):
        received(pr.at[h], pl.ds(0, rows - 1), pl.ds(cuts[h], cuts[h + 1] - cuts[h]))
        if h == 1:
            stage(1, held_back)
        standardize(r, keep_own, range(h * groups // 2, (h + 1) * groups // 2))
        side = slice(h * width // 2, (h + 1) * width // 2)
        sums = sums + lax.dot_general(lhs[:, side], lhs[k:, side], NT, preferred_element_type=jnp.float32)
    summed = jnp.concatenate([sums[:half], sums[half:]], axis=1)
    mine[...] = summed
    for d in range(1, mates):
        pltpu.make_async_remote_copy(
            src_ref=mine, dst_ref=quad.at[m], send_sem=qs.at[0], recv_sem=qr.at[0],
            device_id=mate_id(mate(d)), device_id_type=MESH).start()
    quad[m] = summed
    stage(2)
    others = pltpu.make_async_remote_copy(
        src_ref=quad.at[pl.ds(0, mates - 1)], dst_ref=quad.at[pl.ds(0, mates - 1)],
        send_sem=qs.at[0], recv_sem=qr.at[0], device_id=mate_id(mate(1)), device_id_type=MESH)
    others.wait_recv()
    both = quad[0]
    for q in range(1, mates):
        both = both + quad[q]
    both = jnp.concatenate([both[:, :total], both[:, total:]], axis=0)
    proj, corr = both[:k], both[k:]
    image = exact(proj, corr)
    for step in range(ITERS):
        gram = lax.dot_general(image, proj, NT, precision=HIGHEST,
                               preferred_element_type=jnp.float32) / assets
        if step < ITERS - 1:
            proj, image = eliminate(gram, [image, exact(image, corr)])
        else:
            proj, = eliminate(gram, [proj])
    high = proj.astype(jnp.bfloat16)
    low = (proj - high.astype(jnp.float32)).astype(jnp.bfloat16)
    mix[r] = jnp.concatenate([high, low], axis=0)

    def deliver(slot, q):
        return pltpu.make_async_remote_copy(
            src_ref=mix.at[slot], dst_ref=mix.at[slot], send_sem=ms.at[0], recv_sem=mr.at[slot],
            device_id=row_id(q), device_id_type=MESH)

    def spread(x):
        for q in range(rows):
            if x in wanted(windows, q):
                deliver(x, q).start()

    per_row(spread)
    stage(3)

    def loadings(w, scaled):
        wide = jnp.dot(mix[w], scaled, preferred_element_type=jnp.float32)
        return (wide[:k] + wide[k:]).astype(jnp.bfloat16)

    part = width // PIECES

    def hand(h, side):
        return pltpu.make_async_remote_copy(
            src_ref=made.at[h], dst_ref=got.at[side, h], send_sem=hs.at[0], recv_sem=hr.at[side, h],
            device_id=row_id(r + 1 - 2 * side), device_id_type=MESH)

    def inner(row):
        return jnp.logical_and(row > 0, row < rows - 1)

    for h in range(PIECES):
        some = slice(h * part, (h + 1) * part)
        value = loadings(r, lhs[k:, some])
        made[h] = value

        @pl.when(inner(r))
        def _():
            for side in (0, 1):
                hand(h, side).start()

        out_ref[r, :, some] = value.astype(jnp.float32)

    lists = [wanted(windows, x)[::1 if x in (0, rows - 1) else -1] for x in range(rows)]
    most = max(len(v) for v in lists)
    for act in ("scale", "expand"):
        for j in range(most):
            have = [x for x in range(rows) if len(lists[x]) > j]
            w = sum(jnp.where(r == x, lists[x][j], 0) for x in have)

            @pl.when(functools.reduce(jnp.logical_or, [r == x for x in have]))
            def _():
                if act == "expand":
                    deliver(w, w).wait_recv()
                    out_ref[w] = loadings(w, sbuf[j]).astype(jnp.float32)
                    return

                part_only = [x for x in have if any(p[0] != x and p[1] == lists[x][j] for p in plans[x] if p[3] == 3)]
                fewer = functools.reduce(jnp.logical_or, [r == x for x in part_only], False)
                for count, flag in ((rows - 2, fewer), (rows - 1, jnp.logical_not(fewer))):
                    @pl.when(flag)
                    def _():
                        received(cr.at[w], pl.ds(0, count))

                def keep(g, value):
                    sbuf[j, :, lanes(g)] = value

                standardize(w, keep)

    def collect(side):
        for h in range(PIECES):
            hand(h, side).wait_recv()
            out_ref[r - 1 + 2 * side, :, h * part:(h + 1) * part] = got[side, h].astype(jnp.float32)

    for side in (0, 1):
        @pl.when(inner(r - 1 + 2 * side))
        def _():
            collect(side)

    others.wait_send()
    sent(gs.at[0], gains.at[pl.ds(0, rows - 1)])

    def settle(x):
        count = sum(x in wanted(windows, q) for q in range(rows))
        sent(ms.at[0], mix.at[pl.ds(0, count)])
        sent(rest.at[0], codes.at[pl.ds(0, len(plans[x]))])

    per_row(settle)

    @pl.when(inner(r))
    def _():
        sent(hs.at[0], got)


def fused(returns, starts, start_block, rows, cols, subs):
    windows, days, width = returns.shape
    k = start_block.shape[1]
    total = days * rows
    mates = cols * subs
    half = (k + total) // 2
    groups = width // LANES
    f32, bf16 = jnp.float32, jnp.bfloat16
    dma = pltpu.SemaphoreType.DMA
    return pl.pallas_call(
        functools.partial(kernel, rows, cols, subs, width * mates),
        out_shape=pltpu.VMEM(start_block.shape, f32),
        in_specs=[pl.BlockSpec(memory_space=pl.ANY)] * 3,
        out_specs=pl.BlockSpec(memory_space=pltpu.VMEM),
        scratch_shapes=[
            pltpu.VMEM(returns.shape, f32),
            pltpu.VMEM((windows, 1, width), jnp.int32),
            pltpu.VMEM((k, width), f32),
            pltpu.VMEM((rows * windows, groups + 1, days, LANES), jnp.int16),
            pltpu.VMEM((k + total, width), bf16),
            pltpu.VMEM((windows - 2, total, width), bf16),
            pltpu.VMEM((half, 2 * total), f32),
            pltpu.VMEM((mates, half, 2 * total), f32),
            pltpu.VMEM((windows, 2 * k, total), bf16),
            pltpu.VMEM((rows, windows, 1, LANES), f32),
            pltpu.VMEM((PIECES, k, width // PIECES), bf16),
            pltpu.VMEM((2, PIECES, k, width // PIECES), bf16),
            dma((windows,)), dma((2,)),
            dma((1,)), dma((2,)), dma((windows,)), dma((1,)),
            dma((1,)), dma((1,)), dma((1,)), dma((windows,)),
            dma((1,)), dma((1,)), dma((1,)), dma((1,)), dma((2, PIECES)),
            pltpu.SemaphoreType.REGULAR, pltpu.SemaphoreType.REGULAR((2, rows)),
        ],
        compiler_params=pltpu.CompilerParams(collective_id=0, has_side_effects=True),
    )(returns, starts, start_block)


def gram_of(image):
    return jnp.einsum("wkj,wlj->wkl", image, image, precision=HIGHEST)


def project(factors, scaled):
    rounded = factors.astype(jnp.bfloat16)
    return jnp.einsum("wka,wta->wkt", rounded, scaled, preferred_element_type=jnp.float32)


def expand(proj, widened):
    return jnp.einsum("wkt,wta->wka", proj, widened, precision=HIGHEST)


def orthonormal(image, gram, assets):
    lower = jnp.linalg.cholesky(gram / assets)
    return jax.scipy.linalg.solve_triangular(lower, image, lower=True)


def stepwise(returns, starts, start_block, rows, mates):
    windows, days, width = returns.shape
    row_pos = lax.axis_index("rows")
    total_days = days * rows
    day_index = row_pos * days + jnp.arange(days, dtype=jnp.int32)
    live = (day_index[None, :, None] >= starts[:, None, :]).astype(jnp.float32)
    counts = (total_days - starts).astype(jnp.float32)
    masked = live * returns
    sums = lax.psum(jnp.sum(masked, axis=1), "rows")
    mean = sums / counts
    centered = live * (returns - mean[:, None, :])
    squares = lax.psum(jnp.sum(centered * centered, axis=1), "rows")
    scaled = (centered * lax.rsqrt(squares + 1.0)[:, None, :]).astype(jnp.bfloat16)
    widened = scaled.astype(jnp.float32)
    factors = start_block
    for step in range(ITERS):
        proj = lax.psum(project(factors, scaled), ("cols", "sub"))
        image = lax.psum(expand(proj, widened), "rows")
        gram = lax.psum(gram_of(image), ("cols", "sub"))
        factors = orthonormal(image, gram, width * mates)
    return factors


def on_device(rows, cols, subs, returns, starts, start_block):
    windows, days, width = returns.shape
    k = start_block.shape[1]
    fits = (windows == rows and width == LANES * days and days % 16 == 0 and k % 16 == 0
            and days * rows <= 64 and (days * rows + k) % 16 == 0 and rows == 4 and cols * subs > 1)
    if fits:
        return fused(returns, starts, start_block, rows, cols, subs)
    return stepwise(returns, starts, start_block, rows, cols * subs)


def solution(mesh):
    placed = (
        P("groups", "rows", ("cols", "sub")),
        P("groups", ("cols", "sub")),
        P("groups", None, ("cols", "sub")),
    )
    sizes = (mesh.shape["rows"], mesh.shape["cols"], mesh.shape["sub"])
    return jax.shard_map(
        functools.partial(on_device, *sizes),
        mesh=mesh,
        in_specs=placed,
        out_specs=P("groups", None, ("cols", "sub")),
        check_vma=False,
    )
```

```python
import functools

import jax
import jax.numpy as jnp
from jax import lax
from jax.experimental import pallas as pl
from jax.experimental.pallas import tpu as pltpu
from jax.sharding import PartitionSpec as P

ITERS = 3
HIGHEST = lax.Precision.HIGHEST
MESH = pl.DeviceIdType.MESH
NT = (((1,), (1,)), ((), ()))
SUBLANES = 8
LANES = 128
LIMIT = 6.0
TOP = 32767.0
TINY = 1e-30
PIECES = 2


def eliminate(gram, rights):
    size, wide = gram.shape[0], rights[0].shape[1]
    tiles = size // SUBLANES
    sums = [[x[c * SUBLANES:(c + 1) * SUBLANES] for c in range(tiles)] for x in rights]
    row_id = lax.broadcasted_iota(jnp.int32, (SUBLANES, 1), 0)
    diag = [jnp.ones((SUBLANES, wide), jnp.float32) for _ in range(tiles)]
    panel = {
        (c, i): jnp.broadcast_to(gram[c * SUBLANES:(c + 1) * SUBLANES, i:i + 1], (SUBLANES, wide))
        for i in range(size) for c in range(i // SUBLANES, tiles)
    }
    for i in range(size):
        own, sub = i // SUBLANES, i % SUBLANES
        pivot = panel[own, i][sub:sub + 1]
        inverse = 1.0 / pivot
        diag[own] = jnp.where(row_id == sub, pivot, diag[own])
        ahead = {n: panel[n // SUBLANES, i][n % SUBLANES:n % SUBLANES + 1] for n in range(i + 1, size)}
        rows = [x[own][sub:sub + 1] for x in sums]
        for c in range(own, tiles):
            factor = panel[c, i] * inverse
            if c == own:
                factor = jnp.where(row_id > sub, factor, 0.0)
            for n in range(i + 1, size):
                if c >= n // SUBLANES:
                    panel[c, n] = panel[c, n] - factor * ahead[n]
            for x, row in zip(sums, rows):
                x[c] = x[c] - factor * row
    roots = [lax.rsqrt(d) for d in diag]
    return [jnp.concatenate([v * d for v, d in zip(x, roots)], axis=0) for x in sums]


def exact(left, right):
    return jnp.dot(left, right, precision=HIGHEST, preferred_element_type=jnp.float32)


def wanted(windows, x):
    some = [w for w in range(windows) if w != x and (abs(w - x) > 1 or w in (0, windows - 1))]
    return some if x >= windows // 2 else some[::-1]


def background(rows, windows, x):
    ends = (0, rows - 1)
    plan = []
    for q in range(rows):
        for w in wanted(windows, q) if q != x else []:
            if q in ends:
                plan.append((x, w, q, 0 if abs(q - x) == 1 else 1))
            elif x in ends and abs(q - x) == 1:
                plan.append((x, w, q, 2 if w == x else 0))
            elif abs(q - x) == 1 and abs(w - q) > 1:
                plan.append((x, w, q, 1))
    if x in ends:
        near = 1 if x == 0 else rows - 2
        for s in range(rows):
            if s not in (x, near):
                plan.append((s, x, near, 2))
                plan += [(s, w, near, 3) for w in wanted(windows, near) if w == s]
    return plan


def kernel(rows, cols, subs, assets,
           returns_ref, starts_ref, start_ref, out_ref,
           held, begins, firsts, codes, lhs, sbuf, mine, quad, mix, gains, made, got,
           ls, bs, cs, pr, cr, rr, qs, qr, ms, mr, gs, gr, rest, hs, hr, clear, ready):
    r = lax.axis_index("rows")
    mates = cols * subs
    m = lax.axis_index("cols") * subs + lax.axis_index("sub")
    windows, days, width = returns_ref.shape
    k = start_ref.shape[1]
    total = days * rows
    groups = width // LANES
    half = (k + total) // 2
    def row_peer(d):
        return lax.rem(r + d, rows)

    def mate(d):
        return lax.rem(m + d, mates)

    def row_id(q):
        return {"rows": q}

    def mate_id(q):
        return {"cols": q // subs, "sub": lax.rem(q, subs)}

    def lanes(g):
        return slice(g * LANES, (g + 1) * LANES)

    order = [row_peer(d) for d in sorted(range(rows), key=lambda d: -min(d, rows - d))]
    load_begins = [pltpu.make_async_copy(starts_ref.at[pl.ds(w, 1)], begins.at[w], bs.at[0]) for w in range(windows)]
    for c in load_begins:
        c.start()
    loads = [pltpu.make_async_copy(returns_ref.at[w], held.at[w], ls.at[w]) for w in order]
    for c in loads:
        c.start()
    load_firsts = pltpu.make_async_copy(start_ref.at[r], firsts, bs.at[1])
    load_firsts.start()

    barrier = pltpu.get_barrier_semaphore()
    for step in (1, -1):
        @pl.when(r + step < rows if step > 0 else r > 0)
        def _():
            pl.semaphore_signal(barrier, inc=1, device_id=row_id(r + step), device_id_type=MESH)

    for d in range(1, mates):
        pl.semaphore_signal(barrier, inc=1, device_id=mate_id(mate(d)), device_id_type=MESH)

    cuts = (0, 1 + groups // 2, 1 + groups)

    def received(sem, *region):
        whole = codes.at[region]
        pltpu.make_async_remote_copy(
            src_ref=whole, dst_ref=whole, send_sem=cs.at[0], recv_sem=sem,
            device_id=row_id(row_peer(1)), device_id_type=MESH).wait_recv()

    def sent(sem, ref):
        pltpu.make_async_remote_copy(
            src_ref=ref, dst_ref=ref, send_sem=sem, recv_sem=rr.at[0],
            device_id=row_id(row_peer(1)), device_id_type=MESH).wait_send()

    def half_unit(w, h):
        tiles = codes.at[r * windows + w, pl.ds(cuts[h], cuts[h + 1] - cuts[h])]
        return pltpu.make_async_remote_copy(
            src_ref=tiles, dst_ref=tiles, send_sem=cs.at[0], recv_sem=pr.at[h],
            device_id=row_id(w), device_id_type=MESH)

    def unit(s, w, q, relay):
        return pltpu.make_async_remote_copy(
            src_ref=codes.at[s * windows + w], dst_ref=codes.at[s * windows + w],
            send_sem=rest.at[0], recv_sem=rr.at[0] if relay else cr.at[w],
            device_id=row_id(q), device_id_type=MESH)

    def gain(s, q):
        return pltpu.make_async_remote_copy(
            src_ref=gains.at[s], dst_ref=gains.at[s], send_sem=gs.at[0],
            recv_sem=gr.at[0], device_id=row_id(q), device_id_type=MESH)

    row = lax.broadcasted_iota(jnp.int32, (groups, LANES), 0)
    own_day = r * days + lax.broadcasted_iota(jnp.int32, (days, LANES), 0)

    def encode(w):
        def load(g):
            x = held[w, :, lanes(g)]
            return jnp.where(own_day >= begins[w, :, lanes(g)], x, x[days - 1:days])

        centers = jnp.zeros((groups, LANES), jnp.float32)
        reach = jnp.full((1, LANES), TINY, jnp.float32)
        middles = []
        for g in range(groups):
            x = load(g)
            top = jnp.max(x, axis=0, keepdims=True)
            low = jnp.min(x, axis=0, keepdims=True)
            center = jnp.round((top + low) * (0.5 * TOP / LIMIT))
            middle = center * (LIMIT / TOP)
            reach = jnp.maximum(reach, jnp.maximum(top - middle, middle - low))
            centers = jnp.where(row == g, center, centers)
            middles.append(middle)
        codes[r * windows + w, 0] = centers.astype(jnp.int32).astype(jnp.int16)
        gains[r, w] = reach * (1.0 / TOP)
        inverse = TOP / reach
        for g in range(groups):
            codes[r * windows + w, 1 + g] = jnp.round((load(g) - middles[g]) * inverse).astype(jnp.int32).astype(jnp.int16)

    plans = [background(rows, windows, x) for x in range(rows)]

    def per_row(act):
        for x in range(rows):
            @pl.when(r == x)
            def _():
                act(x)

    def stage(number, some=range(rows)):
        def act(x):
            for s, w, q, when in plans[x]:
                if when == number and x in some:
                    if s != x and w != x:
                        received(rr.at[0], s * windows + w)
                    unit(s, w, q, s == x == w and abs(q - x) == rows - 1).start()

        per_row(act)

    pltpu.make_async_copy(begins, begins, bs.at[0]).wait()
    for i, w in enumerate(order):
        loads[i].wait()
        encode(w)
    pl.semaphore_wait(barrier, mates - 1 + jnp.where(jnp.logical_or(r == 0, r == rows - 1), 1, 2))

    def reach_out(x):
        for t in range(1, rows):
            for step in (1, -1):
                if 0 <= x - step * t < rows and 0 <= x + step < rows and t + 1 < rows:
                    pl.semaphore_signal(ready.at[0 if step > 0 else 1, t + 1], inc=1,
                                        device_id=row_id(x + step), device_id_type=MESH)
            for q in (x + t, x - t):
                if 0 <= q < rows:
                    half_unit(q, 0).start()
                    half_unit(q, 1).start()
                    gain(r, q).start()
            if t == (rows - 1 if x in (0, rows - 1) else 2):
                for s, w, q, when in plans[x]:
                    if when == 0:
                        unit(s, w, q, False).start()
            for side, far in ((0, x - t - 1), (1, x + t + 1)):
                if 0 <= far < rows:
                    pl.semaphore_wait(ready.at[side, t + 1], 1)

    per_row(reach_out)

    load_firsts.wait()
    lhs[:k] = firsts[...].astype(jnp.bfloat16)
    sent(cs.at[0], codes.at[pl.ds(0, rows - 1)])
    for d in range(1, subs):
        pl.semaphore_signal(clear, inc=1, device_id={"sub": lax.rem(lax.axis_index("sub") + d, subs)},
                            device_id_type=MESH)
    pl.semaphore_wait(clear, subs - 1)
    held_back = (0,)
    stage(1, [x for x in range(rows) if x not in held_back])

    day = lax.broadcasted_iota(jnp.int32, (total, LANES), 0)

    def standardize(w, store, some=range(groups)):
        middles = [codes[s * windows + w, 0].astype(jnp.float32) * (LIMIT / TOP) for s in range(rows)]
        steps = [gains[s, w] for s in range(rows)]
        for g in some:
            x = jnp.concatenate([
                codes[s * windows + w, 1 + g].astype(jnp.float32) * steps[s] + middles[s][g:g + 1]
                for s in range(rows)], axis=0)
            begin = begins[w, :, lanes(g)]
            live = day >= begin
            counts = (total - begin).astype(jnp.float32)
            mean = jnp.sum(jnp.where(live, x, 0.0), axis=0, keepdims=True) / counts
            centered = jnp.where(live, x - mean, 0.0)
            squares = jnp.sum(centered * centered, axis=0, keepdims=True)
            store(g, (centered * lax.rsqrt(squares + 1.0)).astype(jnp.bfloat16))

    def keep_own(g, value):
        lhs[k:, lanes(g)] = value

    some_gains = gains.at[pl.ds(0, rows - 1)]
    pltpu.make_async_remote_copy(
        src_ref=some_gains, dst_ref=some_gains, send_sem=gs.at[0], recv_sem=gr.at[0],
        device_id=row_id(row_peer(1)), device_id_type=MESH).wait_recv()
    sums = jnp.zeros((k + total, total), jnp.float32)
    for h in range(2):
        received(pr.at[h], pl.ds(0, rows - 1), pl.ds(cuts[h], cuts[h + 1] - cuts[h]))
        if h == 1:
            stage(1, held_back)
        standardize(r, keep_own, range(h * groups // 2, (h + 1) * groups // 2))
        side = slice(h * width // 2, (h + 1) * width // 2)
        sums = sums + lax.dot_general(lhs[:, side], lhs[k:, side], NT, preferred_element_type=jnp.float32)
    summed = jnp.concatenate([sums[:half], sums[half:]], axis=1)
    mine[...] = summed
    for d in range(1, mates):
        pltpu.make_async_remote_copy(
            src_ref=mine, dst_ref=quad.at[m], send_sem=qs.at[0], recv_sem=qr.at[0],
            device_id=mate_id(mate(d)), device_id_type=MESH).start()
    quad[m] = summed
    stage(2)
    others = pltpu.make_async_remote_copy(
        src_ref=quad.at[pl.ds(0, mates - 1)], dst_ref=quad.at[pl.ds(0, mates - 1)],
        send_sem=qs.at[0], recv_sem=qr.at[0], device_id=mate_id(mate(1)), device_id_type=MESH)
    others.wait_recv()
    both = quad[0]
    for q in range(1, mates):
        both = both + quad[q]
    both = jnp.concatenate([both[:, :total], both[:, total:]], axis=0)
    proj, corr = both[:k], both[k:]
    image = exact(proj, corr)
    for step in range(ITERS):
        gram = lax.dot_general(image, proj, NT, precision=HIGHEST,
                               preferred_element_type=jnp.float32) / assets
        if step < ITERS - 1:
            proj, image = eliminate(gram, [image, exact(image, corr)])
        else:
            proj, = eliminate(gram, [proj])
    high = proj.astype(jnp.bfloat16)
    low = (proj - high.astype(jnp.float32)).astype(jnp.bfloat16)
    mix[r] = jnp.concatenate([high, low], axis=0)

    def deliver(slot, q):
        return pltpu.make_async_remote_copy(
            src_ref=mix.at[slot], dst_ref=mix.at[slot], send_sem=ms.at[0], recv_sem=mr.at[slot],
            device_id=row_id(q), device_id_type=MESH)

    def spread(x):
        for q in range(rows):
            if x in wanted(windows, q):
                deliver(x, q).start()

    per_row(spread)
    stage(3)

    def loadings(w, scaled):
        wide = jnp.dot(mix[w], scaled, preferred_element_type=jnp.float32)
        return (wide[:k] + wide[k:]).astype(jnp.bfloat16)

    part = width // PIECES

    def hand(h, side):
        return pltpu.make_async_remote_copy(
            src_ref=made.at[h], dst_ref=got.at[side, h], send_sem=hs.at[0], recv_sem=hr.at[side, h],
            device_id=row_id(r + 1 - 2 * side), device_id_type=MESH)

    def inner(row):
        return jnp.logical_and(row > 0, row < rows - 1)

    for h in range(PIECES):
        some = slice(h * part, (h + 1) * part)
        value = loadings(r, lhs[k:, some])
        made[h] = value

        @pl.when(inner(r))
        def _():
            for side in (0, 1):
                hand(h, side).start()

        out_ref[r, :, some] = value.astype(jnp.float32)

    lists = [wanted(windows, x)[::1 if x in (0, rows - 1) else -1] for x in range(rows)]
    most = max(len(v) for v in lists)
    for act in ("scale", "expand"):
        for j in range(most):
            have = [x for x in range(rows) if len(lists[x]) > j]
            w = sum(jnp.where(r == x, lists[x][j], 0) for x in have)

            @pl.when(functools.reduce(jnp.logical_or, [r == x for x in have]))
            def _():
                if act == "expand":
                    deliver(w, w).wait_recv()
                    out_ref[w] = loadings(w, sbuf[j]).astype(jnp.float32)
                    return

                part_only = [x for x in have if any(p[0] != x and p[1] == lists[x][j] for p in plans[x] if p[3] == 3)]
                fewer = functools.reduce(jnp.logical_or, [r == x for x in part_only], False)
                for count, flag in ((rows - 2, fewer), (rows - 1, jnp.logical_not(fewer))):
                    @pl.when(flag)
                    def _():
                        received(cr.at[w], pl.ds(0, count))

                def keep(g, value):
                    sbuf[j, :, lanes(g)] = value

                standardize(w, keep)

    def collect(side):
        for h in range(PIECES):
            hand(h, side).wait_recv()
            out_ref[r - 1 + 2 * side, :, h * part:(h + 1) * part] = got[side, h].astype(jnp.float32)

    for side in (0, 1):
        @pl.when(inner(r - 1 + 2 * side))
        def _():
            collect(side)

    others.wait_send()
    sent(gs.at[0], gains.at[pl.ds(0, rows - 1)])

    def settle(x):
        count = sum(x in wanted(windows, q) for q in range(rows))
        sent(ms.at[0], mix.at[pl.ds(0, count)])
        sent(rest.at[0], codes.at[pl.ds(0, len(plans[x]))])

    per_row(settle)

    @pl.when(inner(r))
    def _():
        sent(hs.at[0], got)


def fused(returns, starts, start_block, rows, cols, subs):
    windows, days, width = returns.shape
    k = start_block.shape[1]
    total = days * rows
    mates = cols * subs
    half = (k + total) // 2
    groups = width // LANES
    f32, bf16 = jnp.float32, jnp.bfloat16
    dma = pltpu.SemaphoreType.DMA
    return pl.pallas_call(
        functools.partial(kernel, rows, cols, subs, width * mates),
        out_shape=pltpu.VMEM(start_block.shape, f32),
        in_specs=[pl.BlockSpec(memory_space=pl.ANY)] * 3,
        out_specs=pl.BlockSpec(memory_space=pltpu.VMEM),
        scratch_shapes=[
            pltpu.VMEM(returns.shape, f32),
            pltpu.VMEM((windows, 1, width), jnp.int32),
            pltpu.VMEM((k, width), f32),
            pltpu.VMEM((rows * windows, groups + 1, days, LANES), jnp.int16),
            pltpu.VMEM((k + total, width), bf16),
            pltpu.VMEM((windows - 2, total, width), bf16),
            pltpu.VMEM((half, 2 * total), f32),
            pltpu.VMEM((mates, half, 2 * total), f32),
            pltpu.VMEM((windows, 2 * k, total), bf16),
            pltpu.VMEM((rows, windows, 1, LANES), f32),
            pltpu.VMEM((PIECES, k, width // PIECES), bf16),
            pltpu.VMEM((2, PIECES, k, width // PIECES), bf16),
            dma((windows,)), dma((2,)),
            dma((1,)), dma((2,)), dma((windows,)), dma((1,)),
            dma((1,)), dma((1,)), dma((1,)), dma((windows,)),
            dma((1,)), dma((1,)), dma((1,)), dma((1,)), dma((2, PIECES)),
            pltpu.SemaphoreType.REGULAR, pltpu.SemaphoreType.REGULAR((2, rows)),
        ],
        compiler_params=pltpu.CompilerParams(collective_id=0, has_side_effects=True),
    )(returns, starts, start_block)


def gram_of(image):
    return jnp.einsum("wkj,wlj->wkl", image, image, precision=HIGHEST)


def project(factors, scaled):
    rounded = factors.astype(jnp.bfloat16)
    return jnp.einsum("wka,wta->wkt", rounded, scaled, preferred_element_type=jnp.float32)


def expand(proj, widened):
    return jnp.einsum("wkt,wta->wka", proj, widened, precision=HIGHEST)


def orthonormal(image, gram, assets):
    lower = jnp.linalg.cholesky(gram / assets)
    return jax.scipy.linalg.solve_triangular(lower, image, lower=True)


def stepwise(returns, starts, start_block, rows, mates):
    windows, days, width = returns.shape
    row_pos = lax.axis_index("rows")
    total_days = days * rows
    day_index = row_pos * days + jnp.arange(days, dtype=jnp.int32)
    live = (day_index[None, :, None] >= starts[:, None, :]).astype(jnp.float32)
    counts = (total_days - starts).astype(jnp.float32)
    masked = live * returns
    sums = lax.psum(jnp.sum(masked, axis=1), "rows")
    mean = sums / counts
    centered = live * (returns - mean[:, None, :])
    squares = lax.psum(jnp.sum(centered * centered, axis=1), "rows")
    scaled = (centered * lax.rsqrt(squares + 1.0)[:, None, :]).astype(jnp.bfloat16)
    widened = scaled.astype(jnp.float32)
    factors = start_block
    for step in range(ITERS):
        proj = lax.psum(project(factors, scaled), ("cols", "sub"))
        image = lax.psum(expand(proj, widened), "rows")
        gram = lax.psum(gram_of(image), ("cols", "sub"))
        factors = orthonormal(image, gram, width * mates)
    return factors


def on_device(rows, cols, subs, returns, starts, start_block):
    windows, days, width = returns.shape
    k = start_block.shape[1]
    fits = (windows == rows and width == LANES * days and days % 16 == 0 and k % 16 == 0
            and days * rows <= 64 and (days * rows + k) % 16 == 0 and rows == 4 and cols * subs > 1)
    if fits:
        return fused(returns, starts, start_block, rows, cols, subs)
    return stepwise(returns, starts, start_block, rows, cols * subs)


def solution(mesh):
    placed = (
        P("groups", "rows", ("cols", "sub")),
        P("groups", ("cols", "sub")),
        P("groups", None, ("cols", "sub")),
    )
    sizes = (mesh.shape["rows"], mesh.shape["cols"], mesh.shape["sub"])
    return jax.shard_map(
        functools.partial(on_device, *sizes),
        mesh=mesh,
        in_specs=placed,
        out_specs=P("groups", None, ("cols", "sub")),
        check_vma=False,
    )
```
